256 devices in a mesh: box: 16 (over y_lo, z), dir: 16 (over x, y_hi, core).
Axes of the slice: x: 4, y: 4 (y_hi: 2, y_lo: 2; y = y_hi * 2 + y_lo), z: 8, core: 2. Of those that a mesh axis runs over, the one named last changes fastest.
Arguments:
- sources: float32 [2, 4, 96, 96, 128], P(None, None, 'box', 'dir'), may hold values from -6 to 6
- radiation: float32 [2, 512, 128], replicated, may hold values from -0.5 to 0.5
- interp: float32 [1024, 512], replicated, may hold values from -0.25 to 0.25
- trans_fine: float32 [2, 49, 512], replicated, may hold values from -1.2 to 1.2
- trans_coarse: float32 [2, 49, 1024], replicated, may hold values from -1.2 to 1.2
- child_phase: float32 [4, 1024], replicated, may hold values from -3.140625 to 3.140625
- near_block: float32 [2, 9, 128, 128], replicated, may hold values from -0.5 to 0.5
- far_fine: int32 [96, 96, 49], P('box', 'dir'), may hold values from 0 to 1, as said below
- far_coarse: int32 [48, 48, 49], P('box'), may hold values from 0 to 1, as said below
- near_mask: int32 [96, 96, 9], P('box', 'dir'), may hold values from 0 to 1, as said below
Outputs:
- product: float32 [2, 4, 96, 96, 128], P(None, None, 'box', 'dir')
The draws below stay inside these ranges and needn't reach their ends.
Inputs may be any that keep to these rules, and one draw needn't show every extreme that they name: `far_fine`: flags of displacements within one box (the centre 3 x 3) are 0. `far_coarse`: flags of displacements within one box (the centre 3 x 3) are 0. `near_mask`: the flag of the box itself (index 4) is 1.
All inputs are finite; a program needn't handle non-finite values.
Results may differ from the reference program's by a relative error of at most 0.0001.
Values sent between devices are 32-bit elements; how exact they have to be, the bound alone decides.
A program may use at most 128 MiB of HBM per device.

```python
import math
import jax
import jax.numpy as jnp
from jax import lax

K1 = 512
K2 = 1024
NB = 128
R = 4
GX = 96
GY = 96
GX2 = 48
GY2 = 48


def cycle_flags(key, rows_all, cols_all):
    offsets = jnp.arange(49, dtype=jnp.int32)
    outer = jnp.maximum(jnp.abs(offsets // 7 - 3), jnp.abs(offsets % 7 - 3)) >= 2
    keep = jax.random.randint(key, (rows_all, cols_all, 49), 0, 5) < 3
    return (keep & outer[None, None, :]).astype(jnp.int32)


def draw_far_fine(key, part):
    return cycle_flags(jax.random.fold_in(key, 11), GX, GY)


def draw_far_coarse(key, part):
    return cycle_flags(jax.random.fold_in(key, 12), GX2, GY2)


def draw_near_mask(key, part):
    keep = jax.random.randint(jax.random.fold_in(key, 13), (GX, GY, 9), 0, 4) < 3
    centre = (jnp.arange(9, dtype=jnp.int32) == 4)[None, None, :]
    return (keep | centre).astype(jnp.int32)


def block_levels(key, shape, cuts, low, high):
    gain, own = 1.0, jax.random.fold_in(key, 6)
    for axis_at, blocks in cuts:
        steps = jnp.exp(jax.random.uniform(jax.random.fold_in(own, axis_at), (blocks,), jnp.float32, low / len(cuts), high / len(cuts)))
        gain = gain * jnp.repeat(steps, shape[axis_at] // blocks).reshape([-1 if axis == axis_at else 1 for axis in range(len(shape))])
    return gain


def bell_draw(key, dims, width, limit, cuts=(), kind=jnp.bfloat16):
    array = width * jax.random.normal(key, dims, jnp.float32)
    if cuts:
        array = array * block_levels(key, dims, cuts, -0.22, 0.18)
    return jnp.clip(array, -limit, limit).astype(kind)


def setup_inputs(seed: int = 0) -> dict:
    streams_of = jax.random.split(jax.random.key(seed), 11)
    sources = bell_draw(streams_of[0], (2, R, GX, GY, NB), 1.0, 6.0, ((2, 16), (3, 16)), jnp.float32)
    radiation = bell_draw(streams_of[1], (2, K1, NB), NB ** -0.5, 0.5, (), jnp.float32)
    interp = bell_draw(streams_of[2], (K2, K1), K1 ** -0.5, 0.25, (), jnp.float32)
    trans_fine = bell_draw(streams_of[3], (2, 49, K1), 0.2, 1.2, (), jnp.float32)
    trans_coarse = bell_draw(streams_of[4], (2, 49, K2), 0.2, 1.2, (), jnp.float32)
    child_phase = jnp.clip(jax.random.uniform(streams_of[5], (4, K2), jnp.float32, -3.140625, 3.140625), -3.140625, 3.140625)
    near_block = bell_draw(streams_of[6], (2, 9, NB, NB), NB ** -0.5, 0.5, (), jnp.float32)
    far_fine = draw_far_fine(jax.random.fold_in(streams_of[10], 71), 0)
    far_coarse = draw_far_coarse(jax.random.fold_in(streams_of[10], 71), 0)
    near_mask = draw_near_mask(jax.random.fold_in(streams_of[10], 71), 0)
    return {"sources": sources, "radiation": radiation, "interp": interp, "trans_fine": trans_fine, "trans_coarse": trans_coarse, "child_phase": child_phase, "near_block": near_block, "far_fine": far_fine, "far_coarse": far_coarse, "near_mask": near_mask}


highest = lax.Precision.HIGHEST

def aggregate(sources, radiation):
    real_part = jnp.einsum('...n,kn->...k', sources[0], radiation[0], precision=highest) - jnp.einsum('...n,kn->...k', sources[1], radiation[1], precision=highest)
    imag_part = jnp.einsum('...n,kn->...k', sources[1], radiation[0], precision=highest) + jnp.einsum('...n,kn->...k', sources[0], radiation[1], precision=highest)
    return jnp.stack([real_part, imag_part])

def receive(incoming, radiation):
    scale = 1.0 / math.sqrt(radiation.shape[1])
    real_part = jnp.einsum('...k,kn->...n', incoming[0], radiation[0], precision=highest) + jnp.einsum('...k,kn->...n', incoming[1], radiation[1], precision=highest)
    imag_part = jnp.einsum('...k,kn->...n', incoming[1], radiation[0], precision=highest) - jnp.einsum('...k,kn->...n', incoming[0], radiation[1], precision=highest)
    return jnp.stack([real_part, imag_part]) * scale

def translate(padded, table, listed):
    rows_here = listed.shape[0]
    cols_here = listed.shape[1]
    total_re = jnp.zeros(padded.shape[1:-3] + (rows_here, cols_here, padded.shape[-1]), jnp.float32)
    total_im = total_re
    for offset in range(49):
        row_off = offset // 7 - 3
        col_off = offset % 7 - 3
        if max(abs(row_off), abs(col_off)) < 2:
            continue
        source = padded[..., 3 + row_off:3 + row_off + rows_here, 3 + col_off:3 + col_off + cols_here, :]
        flags = listed[:, :, offset].astype(jnp.float32)[:, :, None]
        table_re = table[0, offset]
        table_im = table[1, offset]
        total_re = total_re + flags * (source[0] * table_re - source[1] * table_im)
        total_im = total_im + flags * (source[0] * table_im + source[1] * table_re)
    return jnp.stack([total_re, total_im])

def interpolate(patterns, interp, child_phase):
    total = None
    for child in range(4):
        row_bit = child // 2
        col_bit = child % 2
        piece = patterns[..., row_bit::2, col_bit::2, :]
        lifted = jnp.einsum('...k,mk->...m', piece, interp, precision=highest)
        cosine = jnp.cos(child_phase[child])
        sine = jnp.sin(child_phase[child])
        shifted = jnp.stack([lifted[0] * cosine - lifted[1] * sine, lifted[0] * sine + lifted[1] * cosine])
        total = shifted if total is None else total + shifted
    return total

def anterpolate(coarse_in, interp, child_phase):
    children = []
    for child in range(4):
        cosine = jnp.cos(child_phase[child])
        sine = jnp.sin(child_phase[child])
        shifted = jnp.stack([coarse_in[0] * cosine + coarse_in[1] * sine, coarse_in[1] * cosine - coarse_in[0] * sine])
        children.append(jnp.einsum('...m,mk->...k', shifted, interp, precision=highest))
    woven = jnp.stack([jnp.stack([children[2 * row_bit + col_bit] for col_bit in (0, 1)], axis=-2) for row_bit in (0, 1)], axis=-4)
    shape = woven.shape
    return woven.reshape(shape[:-5] + (shape[-5] * 2, shape[-3] * 2, shape[-1]))

def nearfield(near_pad, near_block, near_mask):
    rows_here = near_mask.shape[0]
    cols_here = near_mask.shape[1]
    total = None
    for offset in range(9):
        row_off = offset // 3 - 1
        col_off = offset % 3 - 1
        source = near_pad[..., 1 + row_off:1 + row_off + rows_here, 1 + col_off:1 + col_off + cols_here, :]
        flags = near_mask[:, :, offset].astype(jnp.float32)[:, :, None]
        block_re = near_block[0, offset]
        block_im = near_block[1, offset]
        real_part = jnp.einsum('...j,nj->...n', source[0], block_re, precision=highest) - jnp.einsum('...j,nj->...n', source[1], block_im, precision=highest)
        imag_part = jnp.einsum('...j,nj->...n', source[1], block_re, precision=highest) + jnp.einsum('...j,nj->...n', source[0], block_im, precision=highest)
        term = jnp.stack([real_part * flags, imag_part * flags])
        total = term if total is None else total + term
    return total

def reference(sources, radiation, interp, trans_fine, trans_coarse, child_phase, near_block, far_fine, far_coarse, near_mask):

    def one_side(single):
        padded = jnp.pad(aggregate(single, radiation), ((0, 0), (3, 3), (3, 3), (0, 0)))
        patterns = padded[:, 3:-3, 3:-3, :]
        fine_in = translate(padded, trans_fine, far_fine)
        coarse_out = interpolate(patterns, interp, child_phase)
        coarse_pad = jnp.pad(coarse_out, ((0, 0), (3, 3), (3, 3), (0, 0)))
        coarse_in = translate(coarse_pad, trans_coarse, far_coarse)
        incoming = fine_in + anterpolate(coarse_in, interp, child_phase)
        near_pad = jnp.pad(single, ((0, 0), (1, 1), (1, 1), (0, 0)))
        return receive(incoming, radiation) + nearfield(near_pad, near_block, near_mask)
    result = lax.map(one_side, jnp.moveaxis(sources, 1, 0))
    return jnp.moveaxis(result, 0, 1)
```

```python
import math

import jax
import jax.numpy as jnp
from jax import lax
from jax.experimental import pallas as pl
from jax.experimental.pallas import tpu as pltpu
from jax.sharding import PartitionSpec as P

OUTER = [o for o in range(49) if max(abs(o // 7 - 3), abs(o % 7 - 3)) > 1]
F32 = jnp.float32
BF16 = jnp.bfloat16
NN = (((1,), (0,)), ((), ()))
NT = (((1,), (1,)), ((), ()))


def split(x):
    high = x.astype(BF16)
    return high, (x - high.astype(F32)).astype(BF16)


def dot3(a, b, dims):
    a_high, a_low = a
    b_high, b_low = b
    return (
        lax.dot_general(a_high, b_high, dims, preferred_element_type=F32)
        + lax.dot_general(a_low, b_high, dims, preferred_element_type=F32)
        + lax.dot_general(a_high, b_low, dims, preferred_element_type=F32)
    )


def turn(v):
    axis = v.ndim - 2
    rows = lax.broadcasted_iota(jnp.int32, v.shape, axis)
    return jnp.where(rows < 4, -1.0, 1.0) * pltpu.roll(v, 4, axis)


def weights(rad_ref, interp_ref, rad_h, rad_l, wide_h, wide_l):
    for plane in range(2):
        high, low = split(rad_ref[plane])
        rad_h[:, plane * 128 : (plane + 1) * 128] = high
        rad_l[:, plane * 128 : (plane + 1) * 128] = low

    def some(step, _):
        rows = pl.ds(pl.multiple_of(step * 256, 256), 256)
        value = dot3(split(interp_ref[rows, :]), (rad_h[...], rad_l[...]), NN)
        high, low = split(value)
        wide_h[rows, :] = high
        wide_l[rows, :] = low
        return 0

    lax.fori_loop(0, 4, some, 0)


def tables(tf_ref, tc_ref, ff_ref, fc_ref, nm_ref, fine_g, coarse_g, near_g, listed, first):
    for row in range(3):
        for col in range(3):
            listed[3 * row + col : 3 * row + col + 1, 0:49] = fc_ref[
                row, pl.ds(first + col, 1), :
            ].astype(F32)
    flags_c = listed[0:9, 0:49]
    for at, o in enumerate(OUTER):
        flag = jnp.broadcast_to(flags_c[:, o : o + 1], (9, 128))
        for plane in range(2):
            for mt in range(8):
                coarse_g[plane, mt, at * 16 : at * 16 + 9, :] = (
                    flag * tc_ref[o, plane : plane + 1, mt * 128 : (mt + 1) * 128]
                )
    for x in range(6):
        flags = ff_ref[x].astype(F32)
        for at, o in enumerate(OUTER):
            flag = jnp.broadcast_to(flags[:, o : o + 1], (6, 128))
            base = (at * 3 + x % 3) * 8
            for plane in range(2):
                for kt in range(4):
                    fine_g[plane, kt, x // 3, base : base + 6, :] = (
                        flag * tf_ref[o, plane : plane + 1, kt * 128 : (kt + 1) * 128]
                    )
        near = nm_ref[x].astype(F32)
        for o in range(9):
            near_g[o, x, 0:6, :] = jnp.broadcast_to(near[:, o : o + 1], (6, 128))


def arrange(tiles, row, boxes_a, boxes_h, boxes_l):
    def one(x, _):
        parts = []
        for col in range(3):
            re = tiles[row, col, 0, x]
            im = tiles[row, col, 1, x]
            parts.append(jnp.concatenate([re, im], axis=1))
        rows = jnp.concatenate(parts, axis=0)
        turned = turn(rows)
        flat = jnp.concatenate([rows.reshape(144, 128), turned.reshape(144, 128)], axis=1)
        high, low = split(flat)
        at = row * 6 + x
        boxes_a[at] = flat
        boxes_h[at] = high
        boxes_l[at] = low
        return 0

    lax.fori_loop(0, 6, one, 0)


def lift(line, boxes_h, boxes_l, wide_h, wide_l, cosine, sine, coarse):
    a_high = boxes_h[pl.ds(2 * line, 2)].reshape(288, 256)
    a_low = boxes_l[pl.ds(2 * line, 2)].reshape(288, 256)
    for part in range(4):
        cols = slice(part * 256, (part + 1) * 256)
        value = dot3((a_high, a_low), (wide_h[cols, :], wide_l[cols, :]), NT)
        value = value.reshape(2, 9, 2, 8, 256)
        first = None
        for child in range(4):
            piece = value[child // 2, :, child % 2]
            c = piece * cosine[child : child + 1, cols]
            s = piece * sine[child : child + 1, cols]
            first = c if first is None else first + c
            second = s if child == 0 else second + s
        total = (first + turn(second)).reshape(72, 256)
        for half in range(2):
            coarse[2 * part + half, line] = total[:, half * 128 : (half + 1) * 128]


def move_coarse(coarse, coarse_g, coarse_in):
    def one(mt, _):
        plain = [None] * 9
        turned = [None] * 9
        for sx in range(9):
            for sy in range(9):
                value = None
                for bx in range(3):
                    for by in range(3):
                        row_off, col_off = sx - 3 - bx, sy - 3 - by
                        far = max(abs(row_off), abs(col_off))
                        if far > 3 or far < 2:
                            continue
                        at = OUTER.index((row_off + 3) * 7 + col_off + 3)
                        if value is None:
                            value = coarse[mt, sx, sy * 8 : sy * 8 + 8, :]
                        b = bx * 3 + by
                        row = at * 16 + b
                        p = value * coarse_g[0, mt, row : row + 1, :]
                        q = value * coarse_g[1, mt, row : row + 1, :]
                        plain[b] = p if plain[b] is None else plain[b] + p
                        turned[b] = q if turned[b] is None else turned[b] + q
        for b in range(9):
            coarse_in[mt, b * 8 : b * 8 + 8, :] = plain[b] + turn(turned[b])
        return 0

    lax.fori_loop(0, 8, one, 0)


def lower(coarse_in, wide_h, wide_l, cosine, sine, coarse_y):
    for child in range(4):
        total = None
        for part in range(4):
            cols = slice(part * 256, (part + 1) * 256)
            value = jnp.concatenate(
                [coarse_in[2 * part], coarse_in[2 * part + 1]], axis=1
            ).reshape(9, 8, 256)
            shifted = value * cosine[child : child + 1, cols] - turn(value) * sine[
                child : child + 1, cols
            ]
            y = dot3(split(shifted.reshape(72, 256)), (wide_h[cols, :], wide_l[cols, :]), NN)
            total = y if total is None else total + y
        coarse_y[child] = total


def radiate(boxes_h, boxes_l, rad_h, rad_l, fine):
    def one(step, _):
        at = 3 + 3 * step
        a_high = boxes_h[pl.ds(at, 3), 16:128, :].reshape(336, 256)
        a_low = boxes_l[pl.ds(at, 3), 16:128, :].reshape(336, 256)
        for part in range(2):
            cols = slice(part * 256, (part + 1) * 256)
            value = dot3((a_high, a_low), (rad_h[cols, :], rad_l[cols, :]), NT)
            value = value.reshape(3, 112, 256)
            for half in range(2):
                fine[2 * part + half, pl.ds(3 * step, 3)] = value[
                    :, :, half * 128 : (half + 1) * 128
                ]
        return 0

    lax.fori_loop(0, 4, one, 0)


def move_fine(fine, fine_g, fine_in):
    def one(step, _):
        kt = step // 2
        h = step % 2
        plain = [None] * 18
        turned = [None] * 18
        for sx in range(9):
            for sy in range(12):
                value = None
                for bx in range(3):
                    for by in range(6):
                        row_off, col_off = sx - 3 - bx, sy - 3 - by
                        far = max(abs(row_off), abs(col_off))
                        if far > 3 or far < 2:
                            continue
                        at = OUTER.index((row_off + 3) * 7 + col_off + 3)
                        if value is None:
                            value = fine[kt, 3 * h + sx, (sy + 1) * 8 : (sy + 2) * 8, :]
                        b = bx * 6 + by
                        row = (at * 3 + bx) * 8 + by
                        p = value * fine_g[0, kt, h, row : row + 1, :]
                        q = value * fine_g[1, kt, h, row : row + 1, :]
                        plain[b] = p if plain[b] is None else plain[b] + p
                        turned[b] = q if turned[b] is None else turned[b] + q
        for b in range(18):
            fine_in[kt, h, b * 8 : b * 8 + 8, :] = plain[b] + turn(turned[b])
        return 0

    lax.fori_loop(0, 8, one, 0)


def near(boxes_a, nb_ref, near_g, near_y):
    total = [None] * 36
    for col in range(3):
        rows = boxes_a[5:13, (5 + col) * 8 : (11 + col) * 8, :].reshape(384, 256)
        high, low = split(rows)
        for row in range(3):
            o = row * 3 + col
            block = split(jnp.concatenate([nb_ref[0, o], nb_ref[1, o]], axis=1))
            at = slice(48 * row, 48 * row + 288)
            z = dot3((high[at], low[at]), block, NT)
            for b in range(36):
                mask = near_g[o, b // 6, b % 6 : b % 6 + 1, :]
                term = z[b * 8 : b * 8 + 8] * mask
                if o == 0:
                    near_y[b] = term
                else:
                    near_y[b] += term


def finish(fine_in, rad_h, rad_l, coarse_y, near_y, out_ref):
    scale = 1.0 / math.sqrt(512)
    for h in range(2):
        total = None
        for part in range(2):
            cols = slice(part * 256, (part + 1) * 256)
            value = jnp.concatenate([fine_in[2 * part, h], fine_in[2 * part + 1, h]], axis=1)
            y = dot3(split(value), (rad_h[cols, :], rad_l[cols, :]), NN)
            total = y if total is None else total + y
        for b in range(18):
            x, yy = 3 * h + b // 6, b % 6
            child = 2 * (x % 2) + yy % 2
            parent = (x // 2) * 3 + yy // 2
            far = total[b * 8 : b * 8 + 8] + coarse_y[child, parent * 8 : parent * 8 + 8, :]
            value = (far[:, :128] - turn(far[:, 128:])) * scale + near_y[x * 6 + yy]
            out_ref[0, x, yy] = value[0:4]
            out_ref[1, x, yy] = value[4:8]


SCRATCH = dict(
    tiles=((3, 3, 2, 6, 6, 4, 128), F32),
    rad=((2, 512, 128), F32),
    interp=((1024, 512), F32),
    tf=((49, 2, 512), F32),
    tc=((49, 2, 1024), F32),
    phase=((4, 1024), F32),
    blocks=((2, 9, 128, 128), F32),
    ff=((6, 6, 49), jnp.int32),
    fc=((3, 48, 49), jnp.int32),
    nm=((6, 6, 9), jnp.int32),
    rad_h=((512, 256), BF16),
    rad_l=((512, 256), BF16),
    wide_h=((1024, 256), BF16),
    wide_l=((1024, 256), BF16),
    fine_g=((2, 4, 2, 960, 128), F32),
    coarse_g=((2, 8, 640, 128), F32),
    near_g=((9, 6, 8, 128), F32),
    listed=((16, 128), F32),
    boxes_a=((18, 144, 256), F32),
    boxes_h=((18, 144, 256), BF16),
    boxes_l=((18, 144, 256), BF16),
    cosine=((4, 1024), F32),
    sine=((4, 1024), F32),
    coarse=((8, 9, 72, 128), F32),
    coarse_in=((8, 72, 128), F32),
    coarse_y=((4, 72, 256), F32),
    fine=((4, 12, 112, 128), F32),
    fine_in=((4, 2, 144, 128), F32),
    near_y=((36, 8, 128), F32),
)


LOCAL = ("rad", "interp", "tf", "tc", "phase", "blocks", "ff", "fc", "nm")
MESH = pl.DeviceIdType.MESH


def kernel(
    src_ref, rad_ref, interp_ref, tf_ref, tc_ref, ph_ref, nb_ref, ff_ref, fc_ref, nm_ref, out_ref, *scratch
):
    s = dict(zip(SCRATCH, scratch))
    local_sem, own_sem, send_sem, recv_sem = scratch[len(SCRATCH) :]
    tiles = s["tiles"]
    box = lax.axis_index("box")
    col = lax.axis_index("dir")
    boxes_all = lax.axis_size("box")
    cols_all = lax.axis_size("dir")
    core = col % 2
    outer = col - 1 + 2 * core
    partner = col + 1 - 2 * core
    outer_at = 2 * core
    partner_at = 2 - 2 * core
    above = box < boxes_all - 1
    below = box > 0
    beside = jnp.logical_and(col > 0, col < cols_all - 1)

    own = pltpu.make_async_copy(src_ref, tiles.at[1, 1], own_sem)
    own.start()
    given = (rad_ref, interp_ref, tf_ref, tc_ref, ph_ref, nb_ref, ff_ref, fc_ref, nm_ref)
    loads = {
        name: pltpu.make_async_copy(ref, s[name], local_sem.at[at])
        for at, (name, ref) in enumerate(zip(LOCAL, given))
    }
    for name in ("ff", "fc", "nm", "tc", "tf", "phase", "rad", "interp", "blocks"):
        loads[name].start()

    barrier = pltpu.get_barrier_semaphore()
    for cond, where in (
        (above, (box + 1, col)),
        (below, (box - 1, col)),
        (beside, (box, outer)),
        (None, (box, partner)),
    ):
        if cond is None:
            pl.semaphore_signal(barrier, inc=1, device_id=where, device_id_type=MESH)
        else:

            @pl.when(cond)
            def _(where=where):
                pl.semaphore_signal(barrier, inc=1, device_id=where, device_id_type=MESH)

    peers = 1 + sum(jnp.where(cond, 1, 0) for cond in (above, below, beside))
    pl.semaphore_wait(barrier, peers)

    def copies(at, here, there, where):
        return [
            pltpu.make_async_remote_copy(
                src_ref=tiles.at[here[0], here[1], plane],
                dst_ref=tiles.at[there[0], there[1], plane],
                send_sem=send_sem.at[at, plane],
                recv_sem=recv_sem.at[at, plane],
                device_id=where,
                device_id_type=MESH,
            )
            for plane in range(2)
        ]

    to_outer = copies(0, (1, 1), (1, partner_at), (box, outer))
    to_above = copies(1, (1, 1), (0, 1), (box + 1, col))
    to_below = copies(2, (1, 1), (2, 1), (box - 1, col))
    to_partner = copies(3, (1, 1), (1, outer_at), (box, partner))
    relay_above = copies(4, (1, outer_at), (0, outer_at), (box + 1, col))
    relay_below = copies(5, (1, outer_at), (2, outer_at), (box - 1, col))
    pass_low = copies(6, (0, 1), (0, outer_at), (box, partner))
    pass_high = copies(7, (2, 1), (2, outer_at), (box, partner))
    from_outer = copies(0, (1, 1), (1, outer_at), (box, outer))
    from_below = to_above
    from_above = to_below

    own.wait()

    @pl.when(beside)
    def _():
        for c in to_outer:
            c.start()

    @pl.when(above)
    def _():
        for c in to_above:
            c.start()

    @pl.when(below)
    def _():
        for c in to_below:
            c.start()

    for c in to_partner:
        c.start()

    @pl.when(jnp.logical_not(below))
    def _():
        tiles[0] = jnp.zeros(tiles.shape[1:], F32)

    @pl.when(jnp.logical_not(above))
    def _():
        tiles[2] = jnp.zeros(tiles.shape[1:], F32)

    for edge, at in ((0, 0), (cols_all - 1, 2)):

        @pl.when(col == edge)
        def _(at=at):
            tiles[:, at] = jnp.zeros((3,) + tiles.shape[2:], F32)

    for name in ("ff", "fc", "nm", "tc", "tf"):
        loads[name].wait()
    tables(
        s["tf"], s["tc"], s["ff"], s["fc"], s["nm"], s["fine_g"], s["coarse_g"], s["near_g"], s["listed"],
        col * 3,
    )

    @pl.when(below)
    def _():
        for c in from_below:
            c.wait_recv()
        for c in pass_low:
            c.start()

    @pl.when(above)
    def _():
        for c in from_above:
            c.wait_recv()
        for c in pass_high:
            c.start()

    for name in ("phase", "rad", "interp", "blocks"):
        loads[name].wait()
    s["cosine"][...] = jnp.cos(s["phase"][...])
    s["sine"][...] = jnp.sin(s["phase"][...])
    weights(s["rad"], s["interp"], s["rad_h"], s["rad_l"], s["wide_h"], s["wide_l"])

    for plane in range(2):

        @pl.when(beside)
        def _(plane=plane):
            from_outer[plane].wait_recv()

            @pl.when(above)
            def _():
                relay_above[plane].start()

            @pl.when(below)
            def _():
                relay_below[plane].start()

    for c in to_partner:
        c.wait()

    @pl.when(below)
    def _():
        for c in pass_low:
            c.wait()

    @pl.when(above)
    def _():
        for c in pass_high:
            c.wait()

    @pl.when(jnp.logical_and(beside, below))
    def _():
        for c in relay_above:
            c.wait_recv()

    @pl.when(jnp.logical_and(beside, above))
    def _():
        for c in relay_below:
            c.wait_recv()

    for row in range(3):
        arrange(tiles, row, s["boxes_a"], s["boxes_h"], s["boxes_l"])

    def line(i, _):
        lift(i, s["boxes_h"], s["boxes_l"], s["wide_h"], s["wide_l"], s["cosine"], s["sine"], s["coarse"])
        return 0

    lax.fori_loop(0, 9, line, 0)
    radiate(s["boxes_h"], s["boxes_l"], s["rad_h"], s["rad_l"], s["fine"])
    near(s["boxes_a"], s["blocks"], s["near_g"], s["near_y"])
    move_fine(s["fine"], s["fine_g"], s["fine_in"])
    move_coarse(s["coarse"], s["coarse_g"], s["coarse_in"])
    lower(s["coarse_in"], s["wide_h"], s["wide_l"], s["cosine"], s["sine"], s["coarse_y"])
    finish(s["fine_in"], s["rad_h"], s["rad_l"], s["coarse_y"], s["near_y"], out_ref)

    for cond, sent in ((beside, to_outer), (above, to_above), (below, to_below)):

        @pl.when(cond)
        def _(sent=sent):
            for c in sent:
                c.wait_send()

    for cond, sent in ((above, relay_above), (below, relay_below)):

        @pl.when(jnp.logical_and(beside, cond))
        def _(sent=sent):
            for c in sent:
                c.wait_send()


def body(
    sources, radiation, interp, trans_fine, trans_coarse, child_phase, near_block, far_fine, far_coarse, near_mask
):
    anywhere = pl.BlockSpec(memory_space=pl.ANY)
    out = pl.pallas_call(
        kernel,
        out_shape=jax.ShapeDtypeStruct((2, 6, 6, 4, 128), F32),
        in_specs=[anywhere] * 10,
        out_specs=pl.BlockSpec(memory_space=pltpu.VMEM),
        scratch_shapes=[pltpu.VMEM(*v) for v in SCRATCH.values()]
        + [
            pltpu.SemaphoreType.DMA((len(LOCAL),)),
            pltpu.SemaphoreType.DMA,
            pltpu.SemaphoreType.DMA((8, 2)),
            pltpu.SemaphoreType.DMA((8, 2)),
        ],
        compiler_params=pltpu.CompilerParams(
            vmem_limit_bytes=60 << 20, collective_id=0, has_side_effects=True
        ),
        name="product",
    )(
        jnp.transpose(sources, (0, 2, 3, 1, 4)),
        radiation,
        interp,
        jnp.transpose(trans_fine, (1, 0, 2)),
        jnp.transpose(trans_coarse, (1, 0, 2)),
        child_phase,
        near_block,
        far_fine,
        far_coarse,
        near_mask,
    )
    return jnp.transpose(out, (0, 3, 1, 2, 4))


def solution(mesh):
    placed = (
        P(None, None, "box", "dir", None),
        P(),
        P(),
        P(),
        P(),
        P(),
        P(),
        P("box", "dir", None),
        P("box", None, None),
        P("box", "dir", None),
    )
    return jax.shard_map(
        body,
        mesh=mesh,
        in_specs=placed,
        out_specs=P(None, None, "box", "dir", None),
        check_vma=False,
    )
```

```python
import math

import jax
import jax.numpy as jnp
from jax import lax
from jax.experimental import pallas as pl
from jax.experimental.pallas import tpu as pltpu
from jax.sharding import PartitionSpec as P

OUTER = [o for o in range(49) if max(abs(o // 7 - 3), abs(o % 7 - 3)) > 1]
F32 = jnp.float32
BF16 = jnp.bfloat16
NN = (((1,), (0,)), ((), ()))
NT = (((1,), (1,)), ((), ()))


def split(x):
    high = x.astype(BF16)
    return high, (x - high.astype(F32)).astype(BF16)


def dot3(a, b, dims):
    a_high, a_low = a
    b_high, b_low = b
    return (
        lax.dot_general(a_high, b_high, dims, preferred_element_type=F32)
        + lax.dot_general(a_low, b_high, dims, preferred_element_type=F32)
        + lax.dot_general(a_high, b_low, dims, preferred_element_type=F32)
    )


def turn(v):
    axis = v.ndim - 2
    rows = lax.broadcasted_iota(jnp.int32, v.shape, axis)
    return jnp.where(rows < 4, -1.0, 1.0) * pltpu.roll(v, 4, axis)


def weights(rad_ref, interp_ref, rad_h, rad_l, wide_h, wide_l):
    for plane in range(2):
        high, low = split(rad_ref[plane])
        rad_h[:, plane * 128 : (plane + 1) * 128] = high
        rad_l[:, plane * 128 : (plane + 1) * 128] = low

    def some(step, _):
        rows = pl.ds(pl.multiple_of(step * 256, 256), 256)
        value = dot3(split(interp_ref[rows, :]), (rad_h[...], rad_l[...]), NN)
        high, low = split(value)
        wide_h[rows, :] = high
        wide_l[rows, :] = low
        return 0

    lax.fori_loop(0, 4, some, 0)


def tables(tf_ref, tc_ref, ff_ref, fc_ref, nm_ref, fine_g, coarse_g, near_g, listed, first):
    for row in range(3):
        for col in range(3):
            listed[3 * row + col : 3 * row + col + 1, 0:49] = fc_ref[
                row, pl.ds(first + col, 1), :
            ].astype(F32)
    flags_c = listed[0:9, 0:49]
    for at, o in enumerate(OUTER):
        flag = jnp.broadcast_to(flags_c[:, o : o + 1], (9, 128))
        for plane in range(2):
            for mt in range(8):
                coarse_g[plane, mt, at * 16 : at * 16 + 9, :] = (
                    flag * tc_ref[o, plane : plane + 1, mt * 128 : (mt + 1) * 128]
                )
    for x in range(6):
        flags = ff_ref[x].astype(F32)
        for at, o in enumerate(OUTER):
            flag = jnp.broadcast_to(flags[:, o : o + 1], (6, 128))
            base = (at * 3 + x % 3) * 8
            for plane in range(2):
                for kt in range(4):
                    fine_g[plane, kt, x // 3, base : base + 6, :] = (
                        flag * tf_ref[o, plane : plane + 1, kt * 128 : (kt + 1) * 128]
                    )
        near = nm_ref[x].astype(F32)
        for o in range(9):
            near_g[o, x, 0:6, :] = jnp.broadcast_to(near[:, o : o + 1], (6, 128))


def arrange(tiles, row, col, boxes_a, boxes_h, boxes_l):
    def one(x, _):
        rows = jnp.concatenate([tiles[row, col, 0, x], tiles[row, col, 1, x]], axis=1)
        flat = jnp.concatenate([rows.reshape(48, 128), turn(rows).reshape(48, 128)], axis=1)
        high, low = split(flat)
        at = row * 6 + x
        where = pl.ds(pl.multiple_of(col * 48, 16), 48)
        boxes_a[at, where, :] = flat
        boxes_h[at, where, :] = high
        boxes_l[at, where, :] = low
        return 0

    lax.fori_loop(0, 6, one, 0)


def lift(line, lines, col, cols_here, boxes_h, boxes_l, wide_h, wide_l, cosine, sine, coarse):
    at = pl.ds(pl.multiple_of(col * 48, 16), 48 * cols_here)
    count = 96 * lines * cols_here
    a_high = boxes_h[pl.ds(2 * line, 2 * lines), at, :].reshape(count, 256)
    a_low = boxes_l[pl.ds(2 * line, 2 * lines), at, :].reshape(count, 256)
    for part in range(4):
        cols = slice(part * 256, (part + 1) * 256)
        value = dot3((a_high, a_low), (wide_h[cols, :], wide_l[cols, :]), NT)
        value = value.reshape(lines, 2, 3 * cols_here, 2, 8, 256)
        first = None
        for child in range(4):
            piece = value[:, child // 2, :, child % 2]
            c = piece * cosine[child : child + 1, cols]
            s = piece * sine[child : child + 1, cols]
            first = c if first is None else first + c
            second = s if child == 0 else second + s
        total = (first + turn(second)).reshape(lines, 24 * cols_here, 256)
        where = pl.ds(pl.multiple_of(col * 24, 8), 24 * cols_here)
        for half in range(2):
            coarse[2 * part + half, pl.ds(line, lines), where, :] = total[
                :, :, half * 128 : (half + 1) * 128
            ]


def move_coarse(coarse, coarse_g, coarse_in, columns, add):
    def one(mt, _):
        plain = [None] * 9
        turned = [None] * 9
        for sx in range(9):
            for sy in columns:
                value = None
                for bx in range(3):
                    for by in range(3):
                        row_off, col_off = sx - 3 - bx, sy - 3 - by
                        far = max(abs(row_off), abs(col_off))
                        if far > 3 or far < 2:
                            continue
                        at = OUTER.index((row_off + 3) * 7 + col_off + 3)
                        if value is None:
                            value = coarse[mt, sx, sy * 8 : sy * 8 + 8, :]
                        b = bx * 3 + by
                        row = at * 16 + b
                        p = value * coarse_g[0, mt, row : row + 1, :]
                        q = value * coarse_g[1, mt, row : row + 1, :]
                        plain[b] = p if plain[b] is None else plain[b] + p
                        turned[b] = q if turned[b] is None else turned[b] + q
        for b in range(9):
            if plain[b] is None:
                continue
            total = plain[b] + turn(turned[b])
            if add:
                total = total + coarse_in[mt, b * 8 : b * 8 + 8, :]
            coarse_in[mt, b * 8 : b * 8 + 8, :] = total
        return 0

    lax.fori_loop(0, 8, one, 0)


def lower(coarse_in, wide_h, wide_l, cosine, sine, coarse_y):
    for child in range(4):
        total = None
        for part in range(4):
            cols = slice(part * 256, (part + 1) * 256)
            value = jnp.concatenate(
                [coarse_in[2 * part], coarse_in[2 * part + 1]], axis=1
            ).reshape(9, 8, 256)
            shifted = value * cosine[child : child + 1, cols] - turn(value) * sine[
                child : child + 1, cols
            ]
            y = dot3(split(shifted.reshape(72, 256)), (wide_h[cols, :], wide_l[cols, :]), NN)
            total = y if total is None else total + y
        coarse_y[child] = total


def radiate(first, count, per, start, rows, boxes_h, boxes_l, rad_h, rad_l, fine):
    where = pl.ds(pl.multiple_of(start, 16), rows)
    put = pl.ds(pl.multiple_of(start - 16, 8), rows)

    def one(step, _):
        at = first + per * step
        a_high = boxes_h[pl.ds(at, per), where, :].reshape(per * rows, 256)
        a_low = boxes_l[pl.ds(at, per), where, :].reshape(per * rows, 256)
        for part in range(2):
            cols = slice(part * 256, (part + 1) * 256)
            value = dot3((a_high, a_low), (rad_h[cols, :], rad_l[cols, :]), NT)
            value = value.reshape(per, rows, 256)
            for half in range(2):
                fine[2 * part + half, pl.ds(at - 3, per), put, :] = value[
                    :, :, half * 128 : (half + 1) * 128
                ]
        return 0

    lax.fori_loop(0, count // per, one, 0)


def move_fine(fine, fine_g, fine_in, columns, add):
    def one(step, _):
        kt = step // 2
        h = step % 2
        plain = [None] * 18
        turned = [None] * 18
        for sx in range(9):
            for sy in columns:
                value = None
                for bx in range(3):
                    for by in range(6):
                        row_off, col_off = sx - 3 - bx, sy - 3 - by
                        far = max(abs(row_off), abs(col_off))
                        if far > 3 or far < 2:
                            continue
                        at = OUTER.index((row_off + 3) * 7 + col_off + 3)
                        if value is None:
                            value = fine[kt, 3 * h + sx, (sy + 1) * 8 : (sy + 2) * 8, :]
                        b = bx * 6 + by
                        row = (at * 3 + bx) * 8 + by
                        p = value * fine_g[0, kt, h, row : row + 1, :]
                        q = value * fine_g[1, kt, h, row : row + 1, :]
                        plain[b] = p if plain[b] is None else plain[b] + p
                        turned[b] = q if turned[b] is None else turned[b] + q
        for b in range(18):
            if plain[b] is None:
                continue
            total = plain[b] + turn(turned[b])
            if add:
                total = total + fine_in[kt, h, b * 8 : b * 8 + 8, :]
            fine_in[kt, h, b * 8 : b * 8 + 8, :] = total
        return 0

    lax.fori_loop(0, 8, one, 0)


def near(col, add, boxes_a, nb_ref, near_g, near_y):
    rows = boxes_a[5:13, pl.ds(pl.multiple_of((5 + col) * 8, 8), 48), :].reshape(384, 256)
    high, low = split(rows)
    for row in range(3):
        o = row * 3 + col
        block = split(jnp.concatenate([nb_ref[0, o], nb_ref[1, o]], axis=1))
        at = slice(48 * row, 48 * row + 288)
        z = dot3((high[at], low[at]), block, NT)
        for b in range(36):
            term = z[b * 8 : b * 8 + 8] * near_g[o, b // 6, b % 6 : b % 6 + 1, :]
            if row == 0 and not add:
                near_y[b] = term
            else:
                near_y[b] += term


def finish(fine_in, rad_h, rad_l, coarse_y, near_y, out_ref):
    scale = 1.0 / math.sqrt(512)
    for h in range(2):
        total = None
        for part in range(2):
            cols = slice(part * 256, (part + 1) * 256)
            value = jnp.concatenate([fine_in[2 * part, h], fine_in[2 * part + 1, h]], axis=1)
            y = dot3(split(value), (rad_h[cols, :], rad_l[cols, :]), NN)
            total = y if total is None else total + y
        for b in range(18):
            x, yy = 3 * h + b // 6, b % 6
            child = 2 * (x % 2) + yy % 2
            parent = (x // 2) * 3 + yy // 2
            far = total[b * 8 : b * 8 + 8] + coarse_y[child, parent * 8 : parent * 8 + 8, :]
            value = (far[:, :128] - turn(far[:, 128:])) * scale + near_y[x * 6 + yy]
            out_ref[0, x, yy] = value[0:4]
            out_ref[1, x, yy] = value[4:8]


SCRATCH = dict(
    tiles=((3, 3, 2, 6, 6, 4, 128), F32),
    rad=((2, 512, 128), F32),
    interp=((1024, 512), F32),
    tf=((49, 2, 512), F32),
    tc=((49, 2, 1024), F32),
    phase=((4, 1024), F32),
    blocks=((2, 9, 128, 128), F32),
    ff=((6, 6, 49), jnp.int32),
    fc=((3, 48, 49), jnp.int32),
    nm=((6, 6, 9), jnp.int32),
    rad_h=((512, 256), BF16),
    rad_l=((512, 256), BF16),
    wide_h=((1024, 256), BF16),
    wide_l=((1024, 256), BF16),
    fine_g=((2, 4, 2, 960, 128), F32),
    coarse_g=((2, 8, 640, 128), F32),
    near_g=((9, 6, 8, 128), F32),
    listed=((16, 128), F32),
    boxes_a=((18, 144, 256), F32),
    boxes_h=((18, 144, 256), BF16),
    boxes_l=((18, 144, 256), BF16),
    cosine=((4, 1024), F32),
    sine=((4, 1024), F32),
    coarse=((8, 9, 72, 128), F32),
    coarse_in=((8, 72, 128), F32),
    coarse_y=((4, 72, 256), F32),
    fine=((4, 12, 112, 128), F32),
    fine_in=((4, 2, 144, 128), F32),
    near_y=((36, 8, 128), F32),
)


LOCAL = ("rad", "interp", "tf", "tc", "phase", "blocks", "ff", "fc", "nm")
MESH = pl.DeviceIdType.MESH


def kernel(
    src_ref, rad_ref, interp_ref, tf_ref, tc_ref, ph_ref, nb_ref, ff_ref, fc_ref, nm_ref, out_ref, *scratch
):
    s = dict(zip(SCRATCH, scratch))
    local_sem, own_sem, send_sem, recv_sem = scratch[len(SCRATCH) :]
    tiles = s["tiles"]
    box = lax.axis_index("box")
    col = lax.axis_index("dir")
    boxes_all = lax.axis_size("box")
    cols_all = lax.axis_size("dir")
    core = col % 2
    outer = col - 1 + 2 * core
    partner = col + 1 - 2 * core
    outer_at = 2 * core
    partner_at = 2 - 2 * core
    above = box < boxes_all - 1
    below = box > 0
    beside = jnp.logical_and(col > 0, col < cols_all - 1)

    own = pltpu.make_async_copy(src_ref, tiles.at[1, 1], own_sem)
    own.start()
    given = (rad_ref, interp_ref, tf_ref, tc_ref, ph_ref, nb_ref, ff_ref, fc_ref, nm_ref)
    loads = {
        name: pltpu.make_async_copy(ref, s[name], local_sem.at[at])
        for at, (name, ref) in enumerate(zip(LOCAL, given))
    }
    for name in ("ff", "fc", "nm", "tc", "tf", "phase", "rad", "interp", "blocks"):
        loads[name].start()

    barrier = pltpu.get_barrier_semaphore()
    for cond, where in (
        (above, (box + 1, col)),
        (below, (box - 1, col)),
        (beside, (box, outer)),
        (None, (box, partner)),
    ):
        if cond is None:
            pl.semaphore_signal(barrier, inc=1, device_id=where, device_id_type=MESH)
        else:

            @pl.when(cond)
            def _(where=where):
                pl.semaphore_signal(barrier, inc=1, device_id=where, device_id_type=MESH)

    peers = 1 + sum(jnp.where(cond, 1, 0) for cond in (above, below, beside))
    pl.semaphore_wait(barrier, peers)

    def copies(at, here, there, where):
        return [
            pltpu.make_async_remote_copy(
                src_ref=tiles.at[here[0], here[1], plane],
                dst_ref=tiles.at[there[0], there[1], plane],
                send_sem=send_sem.at[at, plane],
                recv_sem=recv_sem.at[at, plane],
                device_id=where,
                device_id_type=MESH,
            )
            for plane in range(2)
        ]

    to_outer = copies(0, (1, 1), (1, partner_at), (box, outer))
    to_above = copies(1, (1, 1), (0, 1), (box + 1, col))
    to_below = copies(2, (1, 1), (2, 1), (box - 1, col))
    to_partner = copies(3, (1, 1), (1, outer_at), (box, partner))
    relay_above = copies(4, (1, outer_at), (0, outer_at), (box + 1, col))
    relay_below = copies(5, (1, outer_at), (2, outer_at), (box - 1, col))
    pass_low = copies(6, (0, 1), (0, outer_at), (box, partner))
    pass_high = copies(7, (2, 1), (2, outer_at), (box, partner))
    from_outer = copies(0, (1, 1), (1, outer_at), (box, outer))
    from_below = to_above
    from_above = to_below

    own.wait()

    @pl.when(beside)
    def _():
        for c in to_outer:
            c.start()

    @pl.when(above)
    def _():
        for c in to_above:
            c.start()

    @pl.when(below)
    def _():
        for c in to_below:
            c.start()

    for c in to_partner:
        c.start()

    @pl.when(jnp.logical_not(below))
    def _():
        tiles[0] = jnp.zeros(tiles.shape[1:], F32)

    @pl.when(jnp.logical_not(above))
    def _():
        tiles[2] = jnp.zeros(tiles.shape[1:], F32)

    for edge, at in ((0, 0), (cols_all - 1, 2)):

        @pl.when(col == edge)
        def _(at=at):
            tiles[:, at] = jnp.zeros((3,) + tiles.shape[2:], F32)

    for name in ("ff", "fc", "nm", "tc", "tf"):
        loads[name].wait()
    tables(
        s["tf"], s["tc"], s["ff"], s["fc"], s["nm"], s["fine_g"], s["coarse_g"], s["near_g"], s["listed"],
        col * 3,
    )

    for name in ("phase", "rad", "interp", "blocks"):
        loads[name].wait()
    s["cosine"][...] = jnp.cos(s["phase"][...])
    s["sine"][...] = jnp.sin(s["phase"][...])

    @pl.when(below)
    def _():
        for c in from_below:
            c.wait_recv()
        for c in pass_low:
            c.start()

    @pl.when(above)
    def _():
        for c in from_above:
            c.wait_recv()
        for c in pass_high:
            c.start()

    weights(s["rad"], s["interp"], s["rad_h"], s["rad_l"], s["wide_h"], s["wide_l"])
    for c in to_partner:
        c.wait()

    @pl.when(below)
    def _():
        for c in pass_low:
            c.wait()

    @pl.when(above)
    def _():
        for c in pass_high:
            c.wait()

    boxes = (s["boxes_a"], s["boxes_h"], s["boxes_l"])
    lifted = (s["boxes_h"], s["boxes_l"], s["wide_h"], s["wide_l"], s["cosine"], s["sine"], s["coarse"])
    sent_out = (s["boxes_h"], s["boxes_l"], s["rad_h"], s["rad_l"], s["fine"])
    close = (s["boxes_a"], s["blocks"], s["near_g"], s["near_y"])
    for row in range(3):
        arrange(tiles, row, 1, *boxes)
        arrange(tiles, row, partner_at, *boxes)

    def line(i, _):
        lift(i, 1, 1 - core, 2, *lifted)
        return 0

    lax.fori_loop(0, 9, line, 0)
    for plane in range(2):

        @pl.when(beside)
        def _(plane=plane):
            from_outer[plane].wait_recv()

            @pl.when(above)
            def _():
                relay_above[plane].start()

            @pl.when(below)
            def _():
                relay_below[plane].start()

    radiate(3, 12, 3, 48 - 32 * core, 80, *sent_out)
    near(1, False, *close)
    near(partner_at, True, *close)
    for side in range(2):

        @pl.when(core == side)
        def _(side=side):
            inner = range(9) if side else range(3, 12)
            move_fine(s["fine"], s["fine_g"], s["fine_in"], inner, False)
            inner = range(6) if side else range(3, 9)
            move_coarse(s["coarse"], s["coarse_g"], s["coarse_in"], inner, False)

    arrange(tiles, 1, outer_at, *boxes)
    lift(3, 3, outer_at, 1, *lifted)

    @pl.when(jnp.logical_and(beside, below))
    def _():
        for c in relay_above:
            c.wait_recv()

    @pl.when(jnp.logical_and(beside, above))
    def _():
        for c in relay_below:
            c.wait_recv()

    arrange(tiles, 0, outer_at, *boxes)
    arrange(tiles, 2, outer_at, *boxes)

    def rest(i, _):
        lift(6 * i, 3, outer_at, 1, *lifted)
        return 0

    lax.fori_loop(0, 2, rest, 0)
    radiate(3, 12, 6, 16 + 80 * core, 32, *sent_out)
    near(outer_at, True, *close)
    for side in range(2):

        @pl.when(core == side)
        def _(side=side):
            outside = range(9, 12) if side else range(3)
            move_fine(s["fine"], s["fine_g"], s["fine_in"], outside, True)
            outside = range(6, 9) if side else range(3)
            move_coarse(s["coarse"], s["coarse_g"], s["coarse_in"], outside, True)

    lower(s["coarse_in"], s["wide_h"], s["wide_l"], s["cosine"], s["sine"], s["coarse_y"])
    finish(s["fine_in"], s["rad_h"], s["rad_l"], s["coarse_y"], s["near_y"], out_ref)

    for cond, sent in ((beside, to_outer), (above, to_above), (below, to_below)):

        @pl.when(cond)
        def _(sent=sent):
            for c in sent:
                c.wait_send()

    for cond, sent in ((above, relay_above), (below, relay_below)):

        @pl.when(jnp.logical_and(beside, cond))
        def _(sent=sent):
            for c in sent:
                c.wait_send()


def body(
    sources, radiation, interp, trans_fine, trans_coarse, child_phase, near_block, far_fine, far_coarse, near_mask
):
    anywhere = pl.BlockSpec(memory_space=pl.ANY)
    out = pl.pallas_call(
        kernel,
        out_shape=jax.ShapeDtypeStruct((2, 6, 6, 4, 128), F32),
        in_specs=[anywhere] * 10,
        out_specs=pl.BlockSpec(memory_space=pltpu.VMEM),
        scratch_shapes=[pltpu.VMEM(*v) for v in SCRATCH.values()]
        + [
            pltpu.SemaphoreType.DMA((len(LOCAL),)),
            pltpu.SemaphoreType.DMA,
            pltpu.SemaphoreType.DMA((8, 2)),
            pltpu.SemaphoreType.DMA((8, 2)),
        ],
        compiler_params=pltpu.CompilerParams(
            vmem_limit_bytes=60 << 20, collective_id=0, has_side_effects=True
        ),
        name="product",
    )(
        jnp.transpose(sources, (0, 2, 3, 1, 4)),
        radiation,
        interp,
        jnp.transpose(trans_fine, (1, 0, 2)),
        jnp.transpose(trans_coarse, (1, 0, 2)),
        child_phase,
        near_block,
        far_fine,
        far_coarse,
        near_mask,
    )
    return jnp.transpose(out, (0, 3, 1, 2, 4))


def solution(mesh):
    placed = (
        P(None, None, "box", "dir", None),
        P(),
        P(),
        P(),
        P(),
        P(),
        P(),
        P("box", "dir", None),
        P("box", None, None),
        P("box", "dir", None),
    )
    return jax.shard_map(
        body,
        mesh=mesh,
        in_specs=placed,
        out_specs=P(None, None, "box", "dir", None),
        check_vma=False,
    )
```

```python
import math

import jax
import jax.numpy as jnp
from jax import lax
from jax.experimental import pallas as pl
from jax.experimental.pallas import tpu as pltpu
from jax.sharding import PartitionSpec as P

OUTER = [o for o in range(49) if max(abs(o // 7 - 3), abs(o % 7 - 3)) > 1]
F32 = jnp.float32
BF16 = jnp.bfloat16
NN = (((1,), (0,)), ((), ()))
NT = (((1,), (1,)), ((), ()))


def split(x):
    high = x.astype(BF16)
    return high, (x - high.astype(F32)).astype(BF16)


def dot3(a, b, dims):
    a_high, a_low = a
    b_high, b_low = b
    return (
        lax.dot_general(a_high, b_high, dims, preferred_element_type=F32)
        + lax.dot_general(a_low, b_high, dims, preferred_element_type=F32)
        + lax.dot_general(a_high, b_low, dims, preferred_element_type=F32)
    )


def turn(v):
    axis = v.ndim - 2
    rows = lax.broadcasted_iota(jnp.int32, v.shape, axis)
    return jnp.where(rows < 4, -1.0, 1.0) * pltpu.roll(v, 4, axis)


def weights(rad_ref, interp_ref, rad_h, rad_l, wide_h, wide_l):
    for plane in range(2):
        high, low = split(rad_ref[plane])
        rad_h[:, plane * 128 : (plane + 1) * 128] = high
        rad_l[:, plane * 128 : (plane + 1) * 128] = low

    def some(step, _):
        rows = pl.ds(pl.multiple_of(step * 512, 512), 512)
        value = dot3(split(interp_ref[rows, :]), (rad_h[...], rad_l[...]), NN)
        high, low = split(value)
        wide_h[rows, :] = high
        wide_l[rows, :] = low
        return 0

    lax.fori_loop(0, 2, some, 0)


def tables(tf_ref, tc_ref, ff_ref, fc_ref, nm_ref, fine_g, coarse_g, near_g, listed, first):
    for row in range(3):
        for col in range(3):
            listed[3 * row + col : 3 * row + col + 1, 0:49] = fc_ref[
                row, pl.ds(first + col, 1), :
            ].astype(F32)
    flags_c = listed[0:9, 0:49]
    for at, o in enumerate(OUTER):
        flag = jnp.broadcast_to(flags_c[:, o : o + 1], (9, 128))
        for plane in range(2):
            for mt in range(8):
                coarse_g[plane, mt, at * 16 : at * 16 + 9, :] = (
                    flag * tc_ref[o, plane : plane + 1, mt * 128 : (mt + 1) * 128]
                )
    for x in range(6):
        flags = ff_ref[x].astype(F32)
        for at, o in enumerate(OUTER):
            flag = jnp.broadcast_to(flags[:, o : o + 1], (6, 128))
            base = (at * 3 + x % 3) * 8
            for plane in range(2):
                for kt in range(4):
                    fine_g[plane, kt, x // 3, base : base + 6, :] = (
                        flag * tf_ref[o, plane : plane + 1, kt * 128 : (kt + 1) * 128]
                    )
        near = nm_ref[x].astype(F32)
        for o in range(9):
            near_g[o, x, 0:6, :] = jnp.broadcast_to(near[:, o : o + 1], (6, 128))


def arrange(tiles, row, col, boxes_a, boxes_h, boxes_l):
    def one(x, _):
        rows = jnp.concatenate([tiles[row, col, 0, x], tiles[row, col, 1, x]], axis=1)
        flat = jnp.concatenate([rows.reshape(48, 128), turn(rows).reshape(48, 128)], axis=1)
        high, low = split(flat)
        at = row * 6 + x
        where = pl.ds(pl.multiple_of(col * 48, 16), 48)
        boxes_a[at, where, :] = flat
        boxes_h[at, where, :] = high
        boxes_l[at, where, :] = low
        return 0

    lax.fori_loop(0, 6, one, 0)


def lift(line, lines, col, cols_here, boxes_h, boxes_l, wide_h, wide_l, cosine, sine, coarse):
    at = pl.ds(pl.multiple_of(col * 48, 16), 48 * cols_here)
    count = 96 * lines * cols_here
    a_high = boxes_h[pl.ds(2 * line, 2 * lines), at, :].reshape(count, 256)
    a_low = boxes_l[pl.ds(2 * line, 2 * lines), at, :].reshape(count, 256)
    for part in range(4):
        cols = slice(part * 256, (part + 1) * 256)
        value = dot3((a_high, a_low), (wide_h[cols, :], wide_l[cols, :]), NT)
        value = value.reshape(lines, 2, 3 * cols_here, 2, 8, 256)
        first = None
        for child in range(4):
            piece = value[:, child // 2, :, child % 2]
            c = piece * cosine[child : child + 1, cols]
            s = piece * sine[child : child + 1, cols]
            first = c if first is None else first + c
            second = s if child == 0 else second + s
        total = (first + turn(second)).reshape(lines, 24 * cols_here, 256)
        where = pl.ds(pl.multiple_of(col * 24, 8), 24 * cols_here)
        for half in range(2):
            coarse[2 * part + half, pl.ds(line, lines), where, :] = total[
                :, :, half * 128 : (half + 1) * 128
            ]


def move_coarse(coarse, coarse_g, coarse_in):
    def one(mt, _):
        plain = [None] * 9
        turned = [None] * 9
        for sx in range(9):
            for sy in range(9):
                value = None
                for bx in range(3):
                    for by in range(3):
                        row_off, col_off = sx - 3 - bx, sy - 3 - by
                        far = max(abs(row_off), abs(col_off))
                        if far > 3 or far < 2:
                            continue
                        at = OUTER.index((row_off + 3) * 7 + col_off + 3)
                        if value is None:
                            value = coarse[mt, sx, sy * 8 : sy * 8 + 8, :]
                        b = bx * 3 + by
                        row = at * 16 + b
                        p = value * coarse_g[0, mt, row : row + 1, :]
                        q = value * coarse_g[1, mt, row : row + 1, :]
                        plain[b] = p if plain[b] is None else plain[b] + p
                        turned[b] = q if turned[b] is None else turned[b] + q
        for b in range(9):
            coarse_in[mt, b * 8 : b * 8 + 8, :] = plain[b] + turn(turned[b])
        return 0

    lax.fori_loop(0, 8, one, 0)


def lower(coarse_in, wide_h, wide_l, cosine, sine, coarse_y):
    total = None
    for part in range(4):
        cols = slice(part * 256, (part + 1) * 256)
        value = jnp.concatenate(
            [coarse_in[2 * part], coarse_in[2 * part + 1]], axis=1
        ).reshape(9, 8, 256)
        other = turn(value)
        shifted = [
            (value * cosine[child : child + 1, cols] - other * sine[child : child + 1, cols]).reshape(72, 256)
            for child in range(4)
        ]
        y = dot3(
            split(jnp.concatenate(shifted, axis=0)), (wide_h[cols, :], wide_l[cols, :]), NN
        )
        total = y if total is None else total + y
    coarse_y[...] = total.reshape(4, 72, 256)


def radiate(first, count, per, start, rows, boxes_h, boxes_l, rad_h, rad_l, fine):
    where = pl.ds(pl.multiple_of(start, 16), rows)
    put = pl.ds(pl.multiple_of(start - 16, 8), rows)

    def one(step, _):
        at = first + per * step
        a_high = boxes_h[pl.ds(at, per), where, :].reshape(per * rows, 256)
        a_low = boxes_l[pl.ds(at, per), where, :].reshape(per * rows, 256)
        for part in range(2):
            cols = slice(part * 256, (part + 1) * 256)
            value = dot3((a_high, a_low), (rad_h[cols, :], rad_l[cols, :]), NT)
            value = value.reshape(per, rows, 256)
            for half in range(2):
                fine[2 * part + half, pl.ds(at - 3, per), put, :] = value[
                    :, :, half * 128 : (half + 1) * 128
                ]
        return 0

    lax.fori_loop(0, count // per, one, 0)


def move_fine(fine, fine_g, fine_in, columns, add):
    def one(step, _):
        kt = step // 2
        h = step % 2
        plain = [None] * 18
        turned = [None] * 18
        for sx in range(9):
            for sy in columns:
                value = None
                for bx in range(3):
                    for by in range(6):
                        row_off, col_off = sx - 3 - bx, sy - 3 - by
                        far = max(abs(row_off), abs(col_off))
                        if far > 3 or far < 2:
                            continue
                        at = OUTER.index((row_off + 3) * 7 + col_off + 3)
                        if value is None:
                            value = fine[kt, 3 * h + sx, (sy + 1) * 8 : (sy + 2) * 8, :]
                        b = bx * 6 + by
                        row = (at * 3 + bx) * 8 + by
                        p = value * fine_g[0, kt, h, row : row + 1, :]
                        q = value * fine_g[1, kt, h, row : row + 1, :]
                        plain[b] = p if plain[b] is None else plain[b] + p
                        turned[b] = q if turned[b] is None else turned[b] + q
        for b in range(18):
            if plain[b] is None:
                continue
            total = plain[b] + turn(turned[b])
            if add:
                total = total + fine_in[kt, h, b * 8 : b * 8 + 8, :]
            fine_in[kt, h, b * 8 : b * 8 + 8, :] = total
        return 0

    lax.fori_loop(0, 8, one, 0)


def near(col, add, boxes_a, nb_ref, near_g, near_y):
    rows = boxes_a[5:13, pl.ds(pl.multiple_of((5 + col) * 8, 8), 48), :].reshape(384, 256)
    high, low = split(rows)
    for row in range(3):
        o = row * 3 + col
        block = split(jnp.concatenate([nb_ref[0, o], nb_ref[1, o]], axis=1))
        at = slice(48 * row, 48 * row + 288)
        z = dot3((high[at], low[at]), block, NT)
        for b in range(36):
            term = z[b * 8 : b * 8 + 8] * near_g[o, b // 6, b % 6 : b % 6 + 1, :]
            if row == 0 and not add:
                near_y[b] = term
            else:
                near_y[b] += term


def finish(fine_in, rad_h, rad_l, coarse_y, near_y, out_ref):
    scale = 1.0 / math.sqrt(512)
    total = None
    for part in range(2):
        cols = slice(part * 256, (part + 1) * 256)
        value = jnp.concatenate(
            [fine_in[2 * part].reshape(288, 128), fine_in[2 * part + 1].reshape(288, 128)], axis=1
        )
        y = dot3(split(value), (rad_h[cols, :], rad_l[cols, :]), NN)
        total = y if total is None else total + y
    for b in range(36):
        x, yy = b // 6, b % 6
        child = 2 * (x % 2) + yy % 2
        parent = (x // 2) * 3 + yy // 2
        far = total[b * 8 : b * 8 + 8] + coarse_y[child, parent * 8 : parent * 8 + 8, :]
        value = (far[:, :128] - turn(far[:, 128:])) * scale + near_y[b]
        out_ref[0, x, yy] = value[0:4]
        out_ref[1, x, yy] = value[4:8]


SCRATCH = dict(
    tiles=((3, 3, 2, 6, 6, 4, 128), F32),
    rad=((2, 512, 128), F32),
    interp=((1024, 512), F32),
    tf=((49, 2, 512), F32),
    tc=((49, 2, 1024), F32),
    phase=((4, 1024), F32),
    blocks=((2, 9, 128, 128), F32),
    ff=((6, 6, 49), jnp.int32),
    fc=((3, 48, 49), jnp.int32),
    nm=((6, 6, 9), jnp.int32),
    rad_h=((512, 256), BF16),
    rad_l=((512, 256), BF16),
    wide_h=((1024, 256), BF16),
    wide_l=((1024, 256), BF16),
    fine_g=((2, 4, 2, 960, 128), F32),
    coarse_g=((2, 8, 640, 128), F32),
    near_g=((9, 6, 8, 128), F32),
    listed=((16, 128), F32),
    boxes_a=((18, 144, 256), F32),
    boxes_h=((18, 144, 256), BF16),
    boxes_l=((18, 144, 256), BF16),
    cosine=((4, 1024), F32),
    sine=((4, 1024), F32),
    coarse=((8, 9, 72, 128), F32),
    coarse_in=((8, 72, 128), F32),
    coarse_y=((4, 72, 256), F32),
    fine=((4, 12, 112, 128), F32),
    fine_in=((4, 2, 144, 128), F32),
    near_y=((36, 8, 128), F32),
)


LOCAL = ("rad", "interp", "tf", "tc", "phase", "blocks", "ff", "fc", "nm")
MESH = pl.DeviceIdType.MESH


def kernel(
    src_ref, rad_ref, interp_ref, tf_ref, tc_ref, ph_ref, nb_ref, ff_ref, fc_ref, nm_ref, out_ref, *scratch
):
    s = dict(zip(SCRATCH, scratch))
    local_sem, own_sem, send_sem, recv_sem, share_sem = scratch[len(SCRATCH) :]
    tiles = s["tiles"]
    box = lax.axis_index("box")
    col = lax.axis_index("dir")
    boxes_all = lax.axis_size("box")
    cols_all = lax.axis_size("dir")
    core = col % 2
    outer = col - 1 + 2 * core
    partner = col + 1 - 2 * core
    outer_at = 2 * core
    partner_at = 2 - 2 * core
    above = box < boxes_all - 1
    below = box > 0
    beside = jnp.logical_and(col > 0, col < cols_all - 1)

    own = pltpu.make_async_copy(src_ref, tiles.at[1, 1], own_sem)
    own.start()
    given = (rad_ref, interp_ref, tf_ref, tc_ref, ph_ref, nb_ref, ff_ref, fc_ref, nm_ref)
    loads = {
        name: pltpu.make_async_copy(ref, s[name], local_sem.at[at])
        for at, (name, ref) in enumerate(zip(LOCAL, given))
    }
    for name in ("ff", "fc", "nm", "tc", "tf", "phase", "rad", "interp", "blocks"):
        loads[name].start()

    barrier = pltpu.get_barrier_semaphore()
    for cond, where in (
        (above, (box + 1, col)),
        (below, (box - 1, col)),
        (beside, (box, outer)),
        (None, (box, partner)),
    ):
        if cond is None:
            pl.semaphore_signal(barrier, inc=1, device_id=where, device_id_type=MESH)
        else:

            @pl.when(cond)
            def _(where=where):
                pl.semaphore_signal(barrier, inc=1, device_id=where, device_id_type=MESH)

    peers = 1 + sum(jnp.where(cond, 1, 0) for cond in (above, below, beside))
    pl.semaphore_wait(barrier, peers)

    def copies(at, here, there, where):
        return [
            pltpu.make_async_remote_copy(
                src_ref=tiles.at[here[0], here[1], plane],
                dst_ref=tiles.at[there[0], there[1], plane],
                send_sem=send_sem.at[at, plane],
                recv_sem=recv_sem.at[at, plane],
                device_id=where,
                device_id_type=MESH,
            )
            for plane in range(2)
        ]

    to_outer = copies(0, (1, 1), (1, partner_at), (box, outer))
    to_above = copies(1, (1, 1), (0, 1), (box + 1, col))
    to_below = copies(2, (1, 1), (2, 1), (box - 1, col))
    to_partner = copies(3, (1, 1), (1, outer_at), (box, partner))
    relay_above = copies(4, (1, outer_at), (0, outer_at), (box + 1, col))
    relay_below = copies(5, (1, outer_at), (2, outer_at), (box - 1, col))
    pass_low = copies(6, (0, 1), (0, outer_at), (box, partner))
    pass_high = copies(7, (2, 1), (2, outer_at), (box, partner))
    from_outer = copies(0, (1, 1), (1, outer_at), (box, outer))
    from_below = to_above
    from_above = to_below

    own.wait()

    lines_z = boxes_all // 2
    late = jnp.logical_or(box % lines_z == 0, box % lines_z == lines_z - 1)

    @pl.when(jnp.logical_and(beside, jnp.logical_not(late)))
    def _():
        for c in to_outer:
            c.start()

    @pl.when(above)
    def _():
        for c in to_above:
            c.start()

    @pl.when(below)
    def _():
        for c in to_below:
            c.start()

    for c in to_partner:
        c.start()

    @pl.when(jnp.logical_not(below))
    def _():
        tiles[0] = jnp.zeros(tiles.shape[1:], F32)

    @pl.when(jnp.logical_not(above))
    def _():
        tiles[2] = jnp.zeros(tiles.shape[1:], F32)

    for edge, at in ((0, 0), (cols_all - 1, 2)):

        @pl.when(col == edge)
        def _(at=at):
            tiles[:, at] = jnp.zeros((3,) + tiles.shape[2:], F32)

    for name in ("ff", "fc", "nm", "tc", "tf"):
        loads[name].wait()
    tables(
        s["tf"], s["tc"], s["ff"], s["fc"], s["nm"], s["fine_g"], s["coarse_g"], s["near_g"], s["listed"],
        col * 3,
    )

    @pl.when(jnp.logical_and(beside, late))
    def _():
        for c in to_outer:
            c.start()

    for name in ("phase", "rad", "interp", "blocks"):
        loads[name].wait()
    s["cosine"][...] = jnp.cos(s["phase"][...])
    s["sine"][...] = jnp.sin(s["phase"][...])

    weights(s["rad"], s["interp"], s["rad_h"], s["rad_l"], s["wide_h"], s["wide_l"])
    boxes = (s["boxes_a"], s["boxes_h"], s["boxes_l"])
    lifted = (s["boxes_h"], s["boxes_l"], s["wide_h"], s["wide_l"], s["cosine"], s["sine"], s["coarse"])
    sent_out = (s["boxes_h"], s["boxes_l"], s["rad_h"], s["rad_l"], s["fine"])
    close = (s["boxes_a"], s["blocks"], s["near_g"], s["near_y"])
    arrange(tiles, 1, 1, *boxes)
    lift(3, 3, 1, 1, *lifted)

    @pl.when(below)
    def _():
        for c in from_below:
            c.wait_recv()
        for c in pass_low:
            c.start()

    @pl.when(above)
    def _():
        for c in from_above:
            c.wait_recv()
        for c in pass_high:
            c.start()

    arrange(tiles, 0, 1, *boxes)
    arrange(tiles, 2, 1, *boxes)

    def ends(i, _):
        lift(6 * i, 3, 1, 1, *lifted)
        return 0

    lax.fori_loop(0, 2, ends, 0)
    for plane in range(2):

        @pl.when(beside)
        def _(plane=plane):
            from_outer[plane].wait_recv()

            @pl.when(above)
            def _():
                relay_above[plane].start()

            @pl.when(below)
            def _():
                relay_below[plane].start()

    for c in to_partner:
        c.wait()
    arrange(tiles, 1, partner_at, *boxes)

    share = pltpu.make_async_remote_copy(
        src_ref=s["coarse"].at[:, :, 24:48, :],
        dst_ref=s["coarse"].at[:, :, pl.ds(pl.multiple_of(24 * outer_at, 8), 24), :],
        send_sem=share_sem.at[0],
        recv_sem=share_sem.at[1],
        device_id=(box, partner),
        device_id_type=MESH,
    )
    share.start()

    @pl.when(below)
    def _():
        for c in pass_low:
            c.wait()

    @pl.when(above)
    def _():
        for c in pass_high:
            c.wait()

    arrange(tiles, 0, partner_at, *boxes)
    arrange(tiles, 2, partner_at, *boxes)
    radiate(3, 12, 6, 48 - 32 * core, 80, *sent_out)
    near(1, False, *close)
    near(partner_at, True, *close)
    for side in range(2):

        @pl.when(core == side)
        def _(side=side):
            inner = range(9) if side else range(3, 12)
            move_fine(s["fine"], s["fine_g"], s["fine_in"], inner, False)

    arrange(tiles, 1, outer_at, *boxes)

    @pl.when(jnp.logical_and(beside, below))
    def _():
        for c in relay_above:
            c.wait_recv()

    @pl.when(jnp.logical_and(beside, above))
    def _():
        for c in relay_below:
            c.wait_recv()

    arrange(tiles, 0, outer_at, *boxes)
    arrange(tiles, 2, outer_at, *boxes)
    lift(0, 9, outer_at, 1, *lifted)
    radiate(3, 12, 12, 16 + 80 * core, 32, *sent_out)
    near(outer_at, True, *close)
    for side in range(2):

        @pl.when(core == side)
        def _(side=side):
            outside = range(9, 12) if side else range(3)
            move_fine(s["fine"], s["fine_g"], s["fine_in"], outside, True)

    share.wait()
    move_coarse(s["coarse"], s["coarse_g"], s["coarse_in"])
    lower(s["coarse_in"], s["wide_h"], s["wide_l"], s["cosine"], s["sine"], s["coarse_y"])
    finish(s["fine_in"], s["rad_h"], s["rad_l"], s["coarse_y"], s["near_y"], out_ref)

    for cond, sent in ((beside, to_outer), (above, to_above), (below, to_below)):

        @pl.when(cond)
        def _(sent=sent):
            for c in sent:
                c.wait_send()

    for cond, sent in ((above, relay_above), (below, relay_below)):

        @pl.when(jnp.logical_and(beside, cond))
        def _(sent=sent):
            for c in sent:
                c.wait_send()


def body(
    sources, radiation, interp, trans_fine, trans_coarse, child_phase, near_block, far_fine, far_coarse, near_mask
):
    anywhere = pl.BlockSpec(memory_space=pl.ANY)
    out = pl.pallas_call(
        kernel,
        out_shape=jax.ShapeDtypeStruct((2, 6, 6, 4, 128), F32),
        in_specs=[anywhere] * 10,
        out_specs=pl.BlockSpec(memory_space=pltpu.VMEM),
        scratch_shapes=[pltpu.VMEM(*v) for v in SCRATCH.values()]
        + [
            pltpu.SemaphoreType.DMA((len(LOCAL),)),
            pltpu.SemaphoreType.DMA,
            pltpu.SemaphoreType.DMA((8, 2)),
            pltpu.SemaphoreType.DMA((8, 2)),
            pltpu.SemaphoreType.DMA((2,)),
        ],
        compiler_params=pltpu.CompilerParams(
            vmem_limit_bytes=60 << 20, collective_id=0, has_side_effects=True
        ),
        name="product",
    )(
        jnp.transpose(sources, (0, 2, 3, 1, 4)),
        radiation,
        interp,
        jnp.transpose(trans_fine, (1, 0, 2)),
        jnp.transpose(trans_coarse, (1, 0, 2)),
        child_phase,
        near_block,
        far_fine,
        far_coarse,
        near_mask,
    )
    return jnp.transpose(out, (0, 3, 1, 2, 4))


def solution(mesh):
    placed = (
        P(None, None, "box", "dir", None),
        P(),
        P(),
        P(),
        P(),
        P(),
        P(),
        P("box", "dir", None),
        P("box", None, None),
        P("box", "dir", None),
    )
    return jax.shard_map(
        body,
        mesh=mesh,
        in_specs=placed,
        out_specs=P(None, None, "box", "dir", None),
        check_vma=False,
    )
```

```python
import math

import jax
import jax.numpy as jnp
from jax import lax
from jax.experimental import pallas as pl
from jax.experimental.pallas import tpu as pltpu
from jax.sharding import PartitionSpec as P

OUTER = [o for o in range(49) if max(abs(o // 7 - 3), abs(o % 7 - 3)) > 1]
F32 = jnp.float32
BF16 = jnp.bfloat16
NN = (((1,), (0,)), ((), ()))
NT = (((1,), (1,)), ((), ()))


def split(x):
    high = x.astype(BF16)
    return high, (x - high.astype(F32)).astype(BF16)


def dot3(a, b, dims):
    a_high, a_low = a
    b_high, b_low = b
    return (
        lax.dot_general(a_high, b_high, dims, preferred_element_type=F32)
        + lax.dot_general(a_low, b_high, dims, preferred_element_type=F32)
        + lax.dot_general(a_high, b_low, dims, preferred_element_type=F32)
    )


def turn(v):
    axis = v.ndim - 2
    rows = lax.broadcasted_iota(jnp.int32, v.shape, axis)
    return jnp.where(rows < 4, -1.0, 1.0) * pltpu.roll(v, 4, axis)


def weights(rad_ref, interp_ref, rad_h, rad_l, wide_h, wide_l):
    for plane in range(2):
        high, low = split(rad_ref[plane])
        rad_h[:, plane * 128 : (plane + 1) * 128] = high
        rad_l[:, plane * 128 : (plane + 1) * 128] = low

    def some(step, _):
        rows = pl.ds(pl.multiple_of(step * 512, 512), 512)
        value = dot3(split(interp_ref[rows, :]), (rad_h[...], rad_l[...]), NN)
        high, low = split(value)
        wide_h[rows, :] = high
        wide_l[rows, :] = low
        return 0

    lax.fori_loop(0, 2, some, 0)


def tables(tf_ref, tc_ref, ff_ref, fc_ref, nm_ref, fine_g, coarse_g, near_g, listed, first):
    for row in range(3):
        for col in range(3):
            listed[3 * row + col : 3 * row + col + 1, 0:49] = fc_ref[
                row, pl.ds(first + col, 1), :
            ].astype(F32)
    flags_c = listed[0:9, 0:49]
    for at, o in enumerate(OUTER):
        flag = jnp.broadcast_to(flags_c[:, o : o + 1], (9, 128))
        for plane in range(2):
            for mt in range(8):
                coarse_g[plane, mt, at * 16 : at * 16 + 9, :] = (
                    flag * tc_ref[o, plane : plane + 1, mt * 128 : (mt + 1) * 128]
                )
    for x in range(6):
        flags = ff_ref[x].astype(F32)
        for at, o in enumerate(OUTER):
            flag = jnp.broadcast_to(flags[:, o : o + 1], (6, 128))
            base = (at * 3 + x % 3) * 8
            for plane in range(2):
                for kt in range(4):
                    fine_g[plane, kt, x // 3, base : base + 6, :] = (
                        flag * tf_ref[o, plane : plane + 1, kt * 128 : (kt + 1) * 128]
                    )
        near = nm_ref[x].astype(F32)
        for o in range(9):
            near_g[o, x, 0:6, :] = jnp.broadcast_to(near[:, o : o + 1], (6, 128))


def arrange(tiles, row, col, boxes_a, boxes_h, boxes_l):
    def one(x, _):
        rows = jnp.concatenate([tiles[row, col, 0, x], tiles[row, col, 1, x]], axis=1)
        flat = jnp.concatenate([rows.reshape(48, 128), turn(rows).reshape(48, 128)], axis=1)
        high, low = split(flat)
        at = row * 6 + x
        where = pl.ds(pl.multiple_of(col * 48, 16), 48)
        boxes_a[at, where, :] = flat
        boxes_h[at, where, :] = high
        boxes_l[at, where, :] = low
        return 0

    lax.fori_loop(0, 6, one, 0)


def lift(line, lines, col, cols_here, boxes_h, boxes_l, wide_h, wide_l, cosine, sine, coarse):
    at = pl.ds(pl.multiple_of(col * 48, 16), 48 * cols_here)
    count = 96 * lines * cols_here
    a_high = boxes_h[pl.ds(2 * line, 2 * lines), at, :].reshape(count, 256)
    a_low = boxes_l[pl.ds(2 * line, 2 * lines), at, :].reshape(count, 256)
    for part in range(4):
        cols = slice(part * 256, (part + 1) * 256)
        value = dot3((a_high, a_low), (wide_h[cols, :], wide_l[cols, :]), NT)
        value = value.reshape(lines, 2, 3 * cols_here, 2, 8, 256)
        first = None
        for child in range(4):
            piece = value[:, child // 2, :, child % 2]
            c = piece * cosine[child : child + 1, cols]
            s = piece * sine[child : child + 1, cols]
            first = c if first is None else first + c
            second = s if child == 0 else second + s
        total = (first + turn(second)).reshape(lines, 24 * cols_here, 256)
        where = pl.ds(pl.multiple_of(col * 24, 8), 24 * cols_here)
        for half in range(2):
            coarse[2 * part + half, pl.ds(line, lines), where, :] = total[
                :, :, half * 128 : (half + 1) * 128
            ]


def move_coarse(coarse, coarse_g, coarse_in):
    def one(mt, _):
        plain = [None] * 9
        turned = [None] * 9
        for sx in range(9):
            for sy in range(9):
                value = None
                for bx in range(3):
                    for by in range(3):
                        row_off, col_off = sx - 3 - bx, sy - 3 - by
                        far = max(abs(row_off), abs(col_off))
                        if far > 3 or far < 2:
                            continue
                        at = OUTER.index((row_off + 3) * 7 + col_off + 3)
                        if value is None:
                            value = coarse[mt, sx, sy * 8 : sy * 8 + 8, :]
                        b = bx * 3 + by
                        row = at * 16 + b
                        p = value * coarse_g[0, mt, row : row + 1, :]
                        q = value * coarse_g[1, mt, row : row + 1, :]
                        plain[b] = p if plain[b] is None else plain[b] + p
                        turned[b] = q if turned[b] is None else turned[b] + q
        for b in range(9):
            coarse_in[mt, b * 8 : b * 8 + 8, :] = plain[b] + turn(turned[b])
        return 0

    lax.fori_loop(0, 8, one, 0)


def lower(coarse_in, wide_h, wide_l, cosine, sine, coarse_y):
    total = None
    for part in range(4):
        cols = slice(part * 256, (part + 1) * 256)
        value = jnp.concatenate(
            [coarse_in[2 * part], coarse_in[2 * part + 1]], axis=1
        ).reshape(9, 8, 256)
        other = turn(value)
        shifted = [
            (value * cosine[child : child + 1, cols] - other * sine[child : child + 1, cols]).reshape(72, 256)
            for child in range(4)
        ]
        y = dot3(
            split(jnp.concatenate(shifted, axis=0)), (wide_h[cols, :], wide_l[cols, :]), NN
        )
        total = y if total is None else total + y
    coarse_y[...] = total.reshape(4, 72, 256)


def radiate(first, stride, steps, per, start, rows, boxes_h, boxes_l, rad_h, rad_l, fine):
    where = pl.ds(pl.multiple_of(start, 16), rows)
    put = pl.ds(pl.multiple_of(start - 16, 8), rows)

    def one(step, _):
        at = first + stride * step
        a_high = boxes_h[pl.ds(at, per), where, :].reshape(per * rows, 256)
        a_low = boxes_l[pl.ds(at, per), where, :].reshape(per * rows, 256)
        for part in range(2):
            cols = slice(part * 256, (part + 1) * 256)
            value = dot3((a_high, a_low), (rad_h[cols, :], rad_l[cols, :]), NT)
            value = value.reshape(per, rows, 256)
            for half in range(2):
                fine[2 * part + half, pl.ds(at - 3, per), put, :] = value[
                    :, :, half * 128 : (half + 1) * 128
                ]
        return 0

    lax.fori_loop(0, steps, one, 0)


def move_fine(fine, fine_g, fine_in, lines, columns, add):
    def one(kt, _):
        for h in range(2):
            plain = [None] * 18
            turned = [None] * 18
            for x in lines:
                for sy in columns:
                    value = None
                    for bx in range(3):
                        for by in range(6):
                            row_off, col_off = x - 3 * h - 3 - bx, sy - 3 - by
                            far = max(abs(row_off), abs(col_off))
                            if far > 3 or far < 2:
                                continue
                            at = OUTER.index((row_off + 3) * 7 + col_off + 3)
                            if value is None:
                                value = fine[kt, x, (sy + 1) * 8 : (sy + 2) * 8, :]
                            b = bx * 6 + by
                            row = (at * 3 + bx) * 8 + by
                            p = value * fine_g[0, kt, h, row : row + 1, :]
                            q = value * fine_g[1, kt, h, row : row + 1, :]
                            plain[b] = p if plain[b] is None else plain[b] + p
                            turned[b] = q if turned[b] is None else turned[b] + q
            for b in range(18):
                if plain[b] is None:
                    continue
                total = plain[b] + turn(turned[b])
                if add:
                    total = total + fine_in[kt, h, b * 8 : b * 8 + 8, :]
                fine_in[kt, h, b * 8 : b * 8 + 8, :] = total
        return 0

    lax.fori_loop(0, 4, one, 0)


def near(col, add, boxes_a, nb_ref, near_g, near_y):
    rows = boxes_a[5:13, pl.ds(pl.multiple_of((5 + col) * 8, 8), 48), :].reshape(384, 256)
    high, low = split(rows)
    for row in range(3):
        o = row * 3 + col
        block = split(jnp.concatenate([nb_ref[0, o], nb_ref[1, o]], axis=1))
        at = slice(48 * row, 48 * row + 288)
        z = dot3((high[at], low[at]), block, NT)
        for b in range(36):
            term = z[b * 8 : b * 8 + 8] * near_g[o, b // 6, b % 6 : b % 6 + 1, :]
            if row == 0 and not add:
                near_y[b] = term
            else:
                near_y[b] += term


def finish(fine_in, rad_h, rad_l, coarse_y, near_y, out_ref):
    scale = 1.0 / math.sqrt(512)
    total = None
    for part in range(2):
        cols = slice(part * 256, (part + 1) * 256)
        value = jnp.concatenate(
            [fine_in[2 * part].reshape(288, 128), fine_in[2 * part + 1].reshape(288, 128)], axis=1
        )
        y = dot3(split(value), (rad_h[cols, :], rad_l[cols, :]), NN)
        total = y if total is None else total + y
    for b in range(36):
        x, yy = b // 6, b % 6
        child = 2 * (x % 2) + yy % 2
        parent = (x // 2) * 3 + yy // 2
        far = total[b * 8 : b * 8 + 8] + coarse_y[child, parent * 8 : parent * 8 + 8, :]
        value = (far[:, :128] - turn(far[:, 128:])) * scale + near_y[b]
        out_ref[0, x, yy] = value[0:4]
        out_ref[1, x, yy] = value[4:8]


SCRATCH = dict(
    tiles=((3, 3, 2, 6, 6, 4, 128), F32),
    rad=((2, 512, 128), F32),
    interp=((1024, 512), F32),
    tf=((49, 2, 512), F32),
    tc=((49, 2, 1024), F32),
    phase=((4, 1024), F32),
    blocks=((2, 9, 128, 128), F32),
    ff=((6, 6, 49), jnp.int32),
    fc=((3, 48, 49), jnp.int32),
    nm=((6, 6, 9), jnp.int32),
    rad_h=((512, 256), BF16),
    rad_l=((512, 256), BF16),
    wide_h=((1024, 256), BF16),
    wide_l=((1024, 256), BF16),
    fine_g=((2, 4, 2, 960, 128), F32),
    coarse_g=((2, 8, 640, 128), F32),
    near_g=((9, 6, 8, 128), F32),
    listed=((16, 128), F32),
    boxes_a=((18, 144, 256), F32),
    boxes_h=((18, 144, 256), BF16),
    boxes_l=((18, 144, 256), BF16),
    cosine=((4, 1024), F32),
    sine=((4, 1024), F32),
    coarse=((8, 9, 72, 128), F32),
    coarse_in=((8, 72, 128), F32),
    coarse_y=((4, 72, 256), F32),
    fine=((4, 12, 112, 128), F32),
    fine_in=((4, 2, 144, 128), F32),
    near_y=((36, 8, 128), F32),
)


LOCAL = ("rad", "interp", "tf", "tc", "phase", "blocks", "ff", "fc", "nm")
MESH = pl.DeviceIdType.MESH


def kernel(
    src_ref, rad_ref, interp_ref, tf_ref, tc_ref, ph_ref, nb_ref, ff_ref, fc_ref, nm_ref, out_ref, *scratch
):
    s = dict(zip(SCRATCH, scratch))
    local_sem, own_sem, send_sem, recv_sem, share_sem = scratch[len(SCRATCH) :]
    tiles = s["tiles"]
    box = lax.axis_index("box")
    col = lax.axis_index("dir")
    boxes_all = lax.axis_size("box")
    cols_all = lax.axis_size("dir")
    core = col % 2
    outer = col - 1 + 2 * core
    partner = col + 1 - 2 * core
    outer_at = 2 * core
    partner_at = 2 - 2 * core
    above = box < boxes_all - 1
    below = box > 0
    beside = jnp.logical_and(col > 0, col < cols_all - 1)

    own = pltpu.make_async_copy(src_ref, tiles.at[1, 1], own_sem)
    own.start()
    given = (rad_ref, interp_ref, tf_ref, tc_ref, ph_ref, nb_ref, ff_ref, fc_ref, nm_ref)
    loads = {
        name: pltpu.make_async_copy(ref, s[name], local_sem.at[at])
        for at, (name, ref) in enumerate(zip(LOCAL, given))
    }
    for name in ("ff", "fc", "nm", "tc", "tf", "phase", "rad", "interp", "blocks"):
        loads[name].start()

    barrier = pltpu.get_barrier_semaphore()
    for cond, where in (
        (above, (box + 1, col)),
        (below, (box - 1, col)),
        (beside, (box, outer)),
        (None, (box, partner)),
    ):
        if cond is None:
            pl.semaphore_signal(barrier, inc=1, device_id=where, device_id_type=MESH)
        else:

            @pl.when(cond)
            def _(where=where):
                pl.semaphore_signal(barrier, inc=1, device_id=where, device_id_type=MESH)

    peers = 1 + sum(jnp.where(cond, 1, 0) for cond in (above, below, beside))
    pl.semaphore_wait(barrier, peers)

    def copies(at, here, there, where):
        return [
            pltpu.make_async_remote_copy(
                src_ref=tiles.at[here[0], here[1], plane],
                dst_ref=tiles.at[there[0], there[1], plane],
                send_sem=send_sem.at[at, plane],
                recv_sem=recv_sem.at[at, plane],
                device_id=where,
                device_id_type=MESH,
            )
            for plane in range(2)
        ]

    to_outer = copies(0, (1, 1), (1, partner_at), (box, outer))
    to_above = copies(1, (1, 1), (0, 1), (box + 1, col))
    to_below = copies(2, (1, 1), (2, 1), (box - 1, col))
    to_partner = copies(3, (1, 1), (1, outer_at), (box, partner))
    relay_above = copies(4, (1, outer_at), (0, outer_at), (box + 1, col))
    relay_below = copies(5, (1, outer_at), (2, outer_at), (box - 1, col))
    pass_low = copies(6, (0, 1), (0, outer_at), (box, partner))
    pass_high = copies(7, (2, 1), (2, outer_at), (box, partner))
    from_outer = copies(0, (1, 1), (1, outer_at), (box, outer))
    from_below = to_above
    from_above = to_below

    own.wait()

    lines_z = boxes_all // 2
    late = jnp.logical_or(box % lines_z == 0, box % lines_z == lines_z - 1)

    @pl.when(jnp.logical_and(beside, jnp.logical_not(late)))
    def _():
        for c in to_outer:
            c.start()

    @pl.when(above)
    def _():
        for c in to_above:
            c.start()

    @pl.when(below)
    def _():
        for c in to_below:
            c.start()

    for c in to_partner:
        c.start()

    @pl.when(jnp.logical_not(below))
    def _():
        tiles[0] = jnp.zeros(tiles.shape[1:], F32)

    @pl.when(jnp.logical_not(above))
    def _():
        tiles[2] = jnp.zeros(tiles.shape[1:], F32)

    for edge, at in ((0, 0), (cols_all - 1, 2)):

        @pl.when(col == edge)
        def _(at=at):
            tiles[:, at] = jnp.zeros((3,) + tiles.shape[2:], F32)

    for name in ("ff", "fc", "nm", "tc", "tf"):
        loads[name].wait()
    tables(
        s["tf"], s["tc"], s["ff"], s["fc"], s["nm"], s["fine_g"], s["coarse_g"], s["near_g"], s["listed"],
        col * 3,
    )

    @pl.when(jnp.logical_and(beside, late))
    def _():
        for c in to_outer:
            c.start()

    for name in ("phase", "rad", "interp", "blocks"):
        loads[name].wait()
    s["cosine"][...] = jnp.cos(s["phase"][...])
    s["sine"][...] = jnp.sin(s["phase"][...])

    weights(s["rad"], s["interp"], s["rad_h"], s["rad_l"], s["wide_h"], s["wide_l"])
    boxes = (s["boxes_a"], s["boxes_h"], s["boxes_l"])
    lifted = (s["boxes_h"], s["boxes_l"], s["wide_h"], s["wide_l"], s["cosine"], s["sine"], s["coarse"])
    sent_out = (s["boxes_h"], s["boxes_l"], s["rad_h"], s["rad_l"], s["fine"])
    close = (s["boxes_a"], s["blocks"], s["near_g"], s["near_y"])
    arrange(tiles, 1, 1, *boxes)
    lift(3, 3, 1, 1, *lifted)

    for c in to_partner:
        c.wait()
    arrange(tiles, 1, partner_at, *boxes)
    radiate(6, 6, 1, 6, 48 - 32 * core, 80, *sent_out)
    for side in range(2):

        @pl.when(core == side)
        def _(side=side):
            inner = range(9) if side else range(3, 12)
            move_fine(s["fine"], s["fine_g"], s["fine_in"], range(3, 9), inner, False)

    for plane in range(2):

        @pl.when(beside)
        def _(plane=plane):
            from_outer[plane].wait_recv()

            @pl.when(above)
            def _():
                relay_above[plane].start()

            @pl.when(below)
            def _():
                relay_below[plane].start()

    @pl.when(below)
    def _():
        for c in from_below:
            c.wait_recv()
        for c in pass_low:
            c.start()

    @pl.when(above)
    def _():
        for c in from_above:
            c.wait_recv()
        for c in pass_high:
            c.start()

    arrange(tiles, 0, 1, *boxes)
    arrange(tiles, 2, 1, *boxes)

    def ends(i, _):
        lift(6 * i, 3, 1, 1, *lifted)
        return 0

    lax.fori_loop(0, 2, ends, 0)
    share = pltpu.make_async_remote_copy(
        src_ref=s["coarse"].at[:, :, 24:48, :],
        dst_ref=s["coarse"].at[:, :, pl.ds(pl.multiple_of(24 * outer_at, 8), 24), :],
        send_sem=share_sem.at[0],
        recv_sem=share_sem.at[1],
        device_id=(box, partner),
        device_id_type=MESH,
    )

    @pl.when(below)
    def _():
        for c in pass_low:
            c.wait()

    @pl.when(above)
    def _():
        for c in pass_high:
            c.wait()

    arrange(tiles, 0, partner_at, *boxes)
    arrange(tiles, 2, partner_at, *boxes)
    share.start()
    radiate(3, 9, 2, 3, 48 - 32 * core, 80, *sent_out)
    near(1, False, *close)
    near(partner_at, True, *close)
    for side in range(2):

        @pl.when(core == side)
        def _(side=side):
            inner = range(9) if side else range(3, 12)
            lines = (0, 1, 2, 9, 10, 11)
            move_fine(s["fine"], s["fine_g"], s["fine_in"], lines, inner, True)

    arrange(tiles, 1, outer_at, *boxes)

    @pl.when(jnp.logical_and(beside, below))
    def _():
        for c in relay_above:
            c.wait_recv()

    @pl.when(jnp.logical_and(beside, above))
    def _():
        for c in relay_below:
            c.wait_recv()

    arrange(tiles, 0, outer_at, *boxes)
    arrange(tiles, 2, outer_at, *boxes)
    lift(0, 9, outer_at, 1, *lifted)
    radiate(3, 12, 1, 12, 16 + 80 * core, 32, *sent_out)
    near(outer_at, True, *close)
    for side in range(2):

        @pl.when(core == side)
        def _(side=side):
            outside = range(9, 12) if side else range(3)
            move_fine(s["fine"], s["fine_g"], s["fine_in"], range(12), outside, True)

    share.wait()
    move_coarse(s["coarse"], s["coarse_g"], s["coarse_in"])
    lower(s["coarse_in"], s["wide_h"], s["wide_l"], s["cosine"], s["sine"], s["coarse_y"])
    finish(s["fine_in"], s["rad_h"], s["rad_l"], s["coarse_y"], s["near_y"], out_ref)

    for cond, sent in ((beside, to_outer), (above, to_above), (below, to_below)):

        @pl.when(cond)
        def _(sent=sent):
            for c in sent:
                c.wait_send()

    for cond, sent in ((above, relay_above), (below, relay_below)):

        @pl.when(jnp.logical_and(beside, cond))
        def _(sent=sent):
            for c in sent:
                c.wait_send()


def body(
    sources, radiation, interp, trans_fine, trans_coarse, child_phase, near_block, far_fine, far_coarse, near_mask
):
    anywhere = pl.BlockSpec(memory_space=pl.ANY)
    out = pl.pallas_call(
        kernel,
        out_shape=jax.ShapeDtypeStruct((2, 6, 6, 4, 128), F32),
        in_specs=[anywhere] * 10,
        out_specs=pl.BlockSpec(memory_space=pltpu.VMEM),
        scratch_shapes=[pltpu.VMEM(*v) for v in SCRATCH.values()]
        + [
            pltpu.SemaphoreType.DMA((len(LOCAL),)),
            pltpu.SemaphoreType.DMA,
            pltpu.SemaphoreType.DMA((8, 2)),
            pltpu.SemaphoreType.DMA((8, 2)),
            pltpu.SemaphoreType.DMA((2,)),
        ],
        compiler_params=pltpu.CompilerParams(
            vmem_limit_bytes=60 << 20, collective_id=0, has_side_effects=True
        ),
        name="product",
    )(
        jnp.transpose(sources, (0, 2, 3, 1, 4)),
        radiation,
        interp,
        jnp.transpose(trans_fine, (1, 0, 2)),
        jnp.transpose(trans_coarse, (1, 0, 2)),
        child_phase,
        near_block,
        far_fine,
        far_coarse,
        near_mask,
    )
    return jnp.transpose(out, (0, 3, 1, 2, 4))


def solution(mesh):
    placed = (
        P(None, None, "box", "dir", None),
        P(),
        P(),
        P(),
        P(),
        P(),
        P(),
        P("box", "dir", None),
        P("box", None, None),
        P("box", "dir", None),
    )
    return jax.shard_map(
        body,
        mesh=mesh,
        in_specs=placed,
        out_specs=P(None, None, "box", "dir", None),
        check_vma=False,
    )
```

```python
import math

import jax
import jax.numpy as jnp
from jax import lax
from jax.experimental import pallas as pl
from jax.experimental.pallas import tpu as pltpu
from jax.sharding import PartitionSpec as P

OUTER = [o for o in range(49) if max(abs(o // 7 - 3), abs(o % 7 - 3)) > 1]
F32 = jnp.float32
BF16 = jnp.bfloat16
NN = (((1,), (0,)), ((), ()))
NT = (((1,), (1,)), ((), ()))


def split(x):
    high = x.astype(BF16)
    return high, (x - high.astype(F32)).astype(BF16)


def dot3(a, b, dims):
    a_high, a_low = a
    b_high, b_low = b
    return (
        lax.dot_general(a_high, b_high, dims, preferred_element_type=F32)
        + lax.dot_general(a_low, b_high, dims, preferred_element_type=F32)
        + lax.dot_general(a_high, b_low, dims, preferred_element_type=F32)
    )


def turn(v):
    axis = v.ndim - 2
    rows = lax.broadcasted_iota(jnp.int32, v.shape, axis)
    return jnp.where(rows < 4, -1.0, 1.0) * pltpu.roll(v, 4, axis)


def weights(rad_ref, interp_ref, rad_h, rad_l, wide_h, wide_l):
    for plane in range(2):
        high, low = split(rad_ref[plane])
        rad_h[:, plane * 128 : (plane + 1) * 128] = high
        rad_l[:, plane * 128 : (plane + 1) * 128] = low

    def some(step, _):
        rows = pl.ds(pl.multiple_of(step * 512, 512), 512)
        value = dot3(split(interp_ref[rows, :]), (rad_h[...], rad_l[...]), NN)
        high, low = split(value)
        wide_h[rows, :] = high
        wide_l[rows, :] = low
        return 0

    lax.fori_loop(0, 2, some, 0)


def tables(tf_ref, tc_ref, ff_ref, fc_ref, nm_ref, fine_g, coarse_g, near_g, listed, first):
    for row in range(3):
        for col in range(3):
            listed[3 * row + col : 3 * row + col + 1, 0:49] = fc_ref[
                row, pl.ds(first + col, 1), :
            ].astype(F32)
    flags_c = listed[0:9, 0:49]
    for at, o in enumerate(OUTER):
        flag = jnp.broadcast_to(flags_c[:, o : o + 1], (9, 128))
        for plane in range(2):
            for mt in range(8):
                coarse_g[plane, mt, at * 16 : at * 16 + 9, :] = (
                    flag * tc_ref[o, plane : plane + 1, mt * 128 : (mt + 1) * 128]
                )
    for x in range(6):
        flags = ff_ref[x].astype(F32)
        for at, o in enumerate(OUTER):
            flag = jnp.broadcast_to(flags[:, o : o + 1], (6, 128))
            base = (at * 3 + x % 3) * 8
            for plane in range(2):
                for kt in range(4):
                    fine_g[plane, kt, x // 3, base : base + 6, :] = (
                        flag * tf_ref[o, plane : plane + 1, kt * 128 : (kt + 1) * 128]
                    )
        near = nm_ref[x].astype(F32)
        for o in range(9):
            near_g[o, x, 0:6, :] = jnp.broadcast_to(near[:, o : o + 1], (6, 128))


def arrange(tiles, row, col, boxes_a, boxes_h, boxes_l):
    def one(x, _):
        rows = jnp.concatenate([tiles[row, col, 0, x], tiles[row, col, 1, x]], axis=1)
        flat = jnp.concatenate([rows.reshape(48, 128), turn(rows).reshape(48, 128)], axis=1)
        high, low = split(flat)
        at = row * 6 + x
        where = pl.ds(pl.multiple_of(col * 48, 16), 48)
        boxes_a[at, where, :] = flat
        boxes_h[at, where, :] = high
        boxes_l[at, where, :] = low
        return 0

    lax.fori_loop(0, 6, one, 0)


def lift(line, lines, col, cols_here, boxes_h, boxes_l, wide_h, wide_l, cosine, sine, coarse):
    at = pl.ds(pl.multiple_of(col * 48, 16), 48 * cols_here)
    count = 96 * lines * cols_here
    a_high = boxes_h[pl.ds(2 * line, 2 * lines), at, :].reshape(count, 256)
    a_low = boxes_l[pl.ds(2 * line, 2 * lines), at, :].reshape(count, 256)
    for part in range(4):
        cols = slice(part * 256, (part + 1) * 256)
        value = dot3((a_high, a_low), (wide_h[cols, :], wide_l[cols, :]), NT)
        value = value.reshape(lines, 2, 3 * cols_here, 2, 8, 256)
        first = None
        for child in range(4):
            piece = value[:, child // 2, :, child % 2]
            c = piece * cosine[child : child + 1, cols]
            s = piece * sine[child : child + 1, cols]
            first = c if first is None else first + c
            second = s if child == 0 else second + s
        total = (first + turn(second)).reshape(lines, 24 * cols_here, 256)
        where = pl.ds(pl.multiple_of(col * 24, 8), 24 * cols_here)
        for half in range(2):
            coarse[2 * part + half, pl.ds(line, lines), where, :] = total[
                :, :, half * 128 : (half + 1) * 128
            ]


def move_coarse(coarse, coarse_g, coarse_in, columns, add):
    def one(mt, _):
        plain = [None] * 9
        turned = [None] * 9
        for sx in range(9):
            for sy in columns:
                value = None
                for bx in range(3):
                    for by in range(3):
                        row_off, col_off = sx - 3 - bx, sy - 3 - by
                        far = max(abs(row_off), abs(col_off))
                        if far > 3 or far < 2:
                            continue
                        at = OUTER.index((row_off + 3) * 7 + col_off + 3)
                        if value is None:
                            value = coarse[mt, sx, sy * 8 : sy * 8 + 8, :]
                        b = bx * 3 + by
                        row = at * 16 + b
                        p = value * coarse_g[0, mt, row : row + 1, :]
                        q = value * coarse_g[1, mt, row : row + 1, :]
                        plain[b] = p if plain[b] is None else plain[b] + p
                        turned[b] = q if turned[b] is None else turned[b] + q
        for b in range(9):
            if plain[b] is None:
                continue
            total = plain[b] + turn(turned[b])
            if add:
                total = total + coarse_in[mt, b * 8 : b * 8 + 8, :]
            coarse_in[mt, b * 8 : b * 8 + 8, :] = total
        return 0

    lax.fori_loop(0, 8, one, 0)


def lower(coarse_in, wide_h, wide_l, cosine, sine, coarse_y):
    total = None
    for part in range(4):
        cols = slice(part * 256, (part + 1) * 256)
        value = jnp.concatenate(
            [coarse_in[2 * part], coarse_in[2 * part + 1]], axis=1
        ).reshape(9, 8, 256)
        other = turn(value)
        shifted = [
            (value * cosine[child : child + 1, cols] - other * sine[child : child + 1, cols]).reshape(72, 256)
            for child in range(4)
        ]
        y = dot3(
            split(jnp.concatenate(shifted, axis=0)), (wide_h[cols, :], wide_l[cols, :]), NN
        )
        total = y if total is None else total + y
    coarse_y[...] = total.reshape(4, 72, 256)


def radiate(first, stride, steps, per, start, rows, boxes_h, boxes_l, rad_h, rad_l, fine):
    where = pl.ds(pl.multiple_of(start, 16), rows)
    put = pl.ds(pl.multiple_of(start - 16, 8), rows)

    def one(step, _):
        at = first + stride * step
        a_high = boxes_h[pl.ds(at, per), where, :].reshape(per * rows, 256)
        a_low = boxes_l[pl.ds(at, per), where, :].reshape(per * rows, 256)
        for part in range(2):
            cols = slice(part * 256, (part + 1) * 256)
            value = dot3((a_high, a_low), (rad_h[cols, :], rad_l[cols, :]), NT)
            value = value.reshape(per, rows, 256)
            for half in range(2):
                fine[2 * part + half, pl.ds(at - 3, per), put, :] = value[
                    :, :, half * 128 : (half + 1) * 128
                ]
        return 0

    lax.fori_loop(0, steps, one, 0)


def move_fine(fine, fine_g, fine_in, lines, columns, add):
    def one(kt, _):
        for h in range(2):
            plain = [None] * 18
            turned = [None] * 18
            for x in lines:
                for sy in columns:
                    value = None
                    for bx in range(3):
                        for by in range(6):
                            row_off, col_off = x - 3 * h - 3 - bx, sy - 3 - by
                            far = max(abs(row_off), abs(col_off))
                            if far > 3 or far < 2:
                                continue
                            at = OUTER.index((row_off + 3) * 7 + col_off + 3)
                            if value is None:
                                value = fine[kt, x, (sy + 1) * 8 : (sy + 2) * 8, :]
                            b = bx * 6 + by
                            row = (at * 3 + bx) * 8 + by
                            p = value * fine_g[0, kt, h, row : row + 1, :]
                            q = value * fine_g[1, kt, h, row : row + 1, :]
                            plain[b] = p if plain[b] is None else plain[b] + p
                            turned[b] = q if turned[b] is None else turned[b] + q
            for b in range(18):
                if plain[b] is None:
                    continue
                total = plain[b] + turn(turned[b])
                if add:
                    total = total + fine_in[kt, h, b * 8 : b * 8 + 8, :]
                fine_in[kt, h, b * 8 : b * 8 + 8, :] = total
        return 0

    lax.fori_loop(0, 4, one, 0)


def near(col, add, boxes_a, nb_ref, near_g, near_y):
    rows = boxes_a[5:13, pl.ds(pl.multiple_of((5 + col) * 8, 8), 48), :].reshape(384, 256)
    high, low = split(rows)
    for row in range(3):
        o = row * 3 + col
        block = split(jnp.concatenate([nb_ref[0, o], nb_ref[1, o]], axis=1))
        at = slice(48 * row, 48 * row + 288)
        z = dot3((high[at], low[at]), block, NT)
        for b in range(36):
            term = z[b * 8 : b * 8 + 8] * near_g[o, b // 6, b % 6 : b % 6 + 1, :]
            if row == 0 and not add:
                near_y[b] = term
            else:
                near_y[b] += term


def finish(fine_in, rad_h, rad_l, coarse_y, near_y, out_ref):
    scale = 1.0 / math.sqrt(512)
    total = None
    for part in range(2):
        cols = slice(part * 256, (part + 1) * 256)
        value = jnp.concatenate(
            [fine_in[2 * part].reshape(288, 128), fine_in[2 * part + 1].reshape(288, 128)], axis=1
        )
        y = dot3(split(value), (rad_h[cols, :], rad_l[cols, :]), NN)
        total = y if total is None else total + y
    for b in range(36):
        x, yy = b // 6, b % 6
        child = 2 * (x % 2) + yy % 2
        parent = (x // 2) * 3 + yy // 2
        far = total[b * 8 : b * 8 + 8] + coarse_y[child, parent * 8 : parent * 8 + 8, :]
        value = (far[:, :128] - turn(far[:, 128:])) * scale + near_y[b]
        out_ref[0, x, yy] = value[0:4]
        out_ref[1, x, yy] = value[4:8]


SCRATCH = dict(
    tiles=((3, 3, 2, 6, 6, 4, 128), F32),
    rad=((2, 512, 128), F32),
    interp=((1024, 512), F32),
    tf=((49, 2, 512), F32),
    tc=((49, 2, 1024), F32),
    phase=((4, 1024), F32),
    blocks=((2, 9, 128, 128), F32),
    ff=((6, 6, 49), jnp.int32),
    fc=((3, 48, 49), jnp.int32),
    nm=((6, 6, 9), jnp.int32),
    rad_h=((512, 256), BF16),
    rad_l=((512, 256), BF16),
    wide_h=((1024, 256), BF16),
    wide_l=((1024, 256), BF16),
    fine_g=((2, 4, 2, 960, 128), F32),
    coarse_g=((2, 8, 640, 128), F32),
    near_g=((9, 6, 8, 128), F32),
    listed=((16, 128), F32),
    boxes_a=((18, 144, 256), F32),
    boxes_h=((18, 144, 256), BF16),
    boxes_l=((18, 144, 256), BF16),
    cosine=((4, 1024), F32),
    sine=((4, 1024), F32),
    coarse=((8, 9, 72, 128), F32),
    coarse_in=((8, 72, 128), F32),
    coarse_y=((4, 72, 256), F32),
    fine=((4, 12, 112, 128), F32),
    fine_in=((4, 2, 144, 128), F32),
    near_y=((36, 8, 128), F32),
)


LOCAL = ("rad", "interp", "tf", "tc", "phase", "blocks", "ff", "fc", "nm")
MESH = pl.DeviceIdType.MESH


def kernel(
    src_ref, rad_ref, interp_ref, tf_ref, tc_ref, ph_ref, nb_ref, ff_ref, fc_ref, nm_ref, out_ref, *scratch
):
    s = dict(zip(SCRATCH, scratch))
    local_sem, own_sem, send_sem, recv_sem, share_sem = scratch[len(SCRATCH) :]
    tiles = s["tiles"]
    box = lax.axis_index("box")
    col = lax.axis_index("dir")
    boxes_all = lax.axis_size("box")
    cols_all = lax.axis_size("dir")
    core = col % 2
    outer = col - 1 + 2 * core
    partner = col + 1 - 2 * core
    outer_at = 2 * core
    partner_at = 2 - 2 * core
    above = box < boxes_all - 1
    below = box > 0
    beside = jnp.logical_and(col > 0, col < cols_all - 1)

    own = pltpu.make_async_copy(src_ref, tiles.at[1, 1], own_sem)
    own.start()
    given = (rad_ref, interp_ref, tf_ref, tc_ref, ph_ref, nb_ref, ff_ref, fc_ref, nm_ref)
    loads = {
        name: pltpu.make_async_copy(ref, s[name], local_sem.at[at])
        for at, (name, ref) in enumerate(zip(LOCAL, given))
    }
    for name in ("ff", "fc", "nm", "tc", "tf", "phase", "rad", "interp", "blocks"):
        loads[name].start()

    barrier = pltpu.get_barrier_semaphore()
    for cond, where in (
        (above, (box + 1, col)),
        (below, (box - 1, col)),
        (beside, (box, outer)),
        (None, (box, partner)),
    ):
        if cond is None:
            pl.semaphore_signal(barrier, inc=1, device_id=where, device_id_type=MESH)
        else:

            @pl.when(cond)
            def _(where=where):
                pl.semaphore_signal(barrier, inc=1, device_id=where, device_id_type=MESH)

    peers = 1 + sum(jnp.where(cond, 1, 0) for cond in (above, below, beside))
    pl.semaphore_wait(barrier, peers)

    def copies(at, here, there, where):
        return [
            pltpu.make_async_remote_copy(
                src_ref=tiles.at[here[0], here[1], plane],
                dst_ref=tiles.at[there[0], there[1], plane],
                send_sem=send_sem.at[at, plane],
                recv_sem=recv_sem.at[at, plane],
                device_id=where,
                device_id_type=MESH,
            )
            for plane in range(2)
        ]

    to_outer = copies(0, (1, 1), (1, partner_at), (box, outer))
    to_above = copies(1, (1, 1), (0, 1), (box + 1, col))
    to_below = copies(2, (1, 1), (2, 1), (box - 1, col))
    to_partner = copies(3, (1, 1), (1, outer_at), (box, partner))
    relay_above = copies(4, (1, outer_at), (0, outer_at), (box + 1, col))
    relay_below = copies(5, (1, outer_at), (2, outer_at), (box - 1, col))
    pass_low = copies(6, (0, 1), (0, outer_at), (box, partner))
    pass_high = copies(7, (2, 1), (2, outer_at), (box, partner))
    from_outer = copies(0, (1, 1), (1, outer_at), (box, outer))
    from_below = to_above
    from_above = to_below

    own.wait()

    lines_z = boxes_all // 2
    late = jnp.logical_or(box % lines_z == 0, box % lines_z == lines_z - 1)

    @pl.when(jnp.logical_and(beside, jnp.logical_not(late)))
    def _():
        for c in to_outer:
            c.start()

    @pl.when(above)
    def _():
        for c in to_above:
            c.start()

    @pl.when(below)
    def _():
        for c in to_below:
            c.start()

    for c in to_partner:
        c.start()

    @pl.when(jnp.logical_not(below))
    def _():
        tiles[0] = jnp.zeros(tiles.shape[1:], F32)

    @pl.when(jnp.logical_not(above))
    def _():
        tiles[2] = jnp.zeros(tiles.shape[1:], F32)

    for edge, at in ((0, 0), (cols_all - 1, 2)):

        @pl.when(col == edge)
        def _(at=at):
            tiles[:, at] = jnp.zeros((3,) + tiles.shape[2:], F32)

    for name in ("ff", "fc", "nm", "tc", "tf"):
        loads[name].wait()
    tables(
        s["tf"], s["tc"], s["ff"], s["fc"], s["nm"], s["fine_g"], s["coarse_g"], s["near_g"], s["listed"],
        col * 3,
    )

    @pl.when(jnp.logical_and(beside, late))
    def _():
        for c in to_outer:
            c.start()

    for name in ("phase", "rad", "interp", "blocks"):
        loads[name].wait()
    s["cosine"][...] = jnp.cos(s["phase"][...])
    s["sine"][...] = jnp.sin(s["phase"][...])

    weights(s["rad"], s["interp"], s["rad_h"], s["rad_l"], s["wide_h"], s["wide_l"])
    boxes = (s["boxes_a"], s["boxes_h"], s["boxes_l"])
    lifted = (s["boxes_h"], s["boxes_l"], s["wide_h"], s["wide_l"], s["cosine"], s["sine"], s["coarse"])
    sent_out = (s["boxes_h"], s["boxes_l"], s["rad_h"], s["rad_l"], s["fine"])
    close = (s["boxes_a"], s["blocks"], s["near_g"], s["near_y"])
    arrange(tiles, 1, 1, *boxes)
    lift(3, 3, 1, 1, *lifted)

    for c in to_partner:
        c.wait()
    arrange(tiles, 1, partner_at, *boxes)
    radiate(6, 6, 1, 6, 48 - 32 * core, 80, *sent_out)
    for side in range(2):

        @pl.when(core == side)
        def _(side=side):
            inner = range(9) if side else range(3, 12)
            move_fine(s["fine"], s["fine_g"], s["fine_in"], range(3, 9), inner, False)

    for plane in range(2):

        @pl.when(beside)
        def _(plane=plane):
            from_outer[plane].wait_recv()

            @pl.when(above)
            def _():
                relay_above[plane].start()

            @pl.when(below)
            def _():
                relay_below[plane].start()

    @pl.when(above)
    def _():
        for c in from_above:
            c.wait_recv()
        for c in pass_high:
            c.start()

    arrange(tiles, 2, 1, *boxes)
    lift(6, 3, 1, 1, *lifted)
    arrange(tiles, 1, outer_at, *boxes)
    lift(3, 3, outer_at, 1, *lifted)

    @pl.when(above)
    def _():
        for c in pass_high:
            c.wait()

    arrange(tiles, 2, partner_at, *boxes)
    radiate(12, 3, 1, 3, 48 - 32 * core, 80, *sent_out)
    for side in range(2):

        @pl.when(core == side)
        def _(side=side):
            inner = range(9) if side else range(3, 12)
            move_fine(s["fine"], s["fine_g"], s["fine_in"], range(9, 12), inner, True)

    @pl.when(below)
    def _():
        for c in from_below:
            c.wait_recv()
        for c in pass_low:
            c.start()

    arrange(tiles, 0, 1, *boxes)
    lift(0, 3, 1, 1, *lifted)
    share = pltpu.make_async_remote_copy(
        src_ref=s["coarse"].at[:, :, 24:48, :],
        dst_ref=s["coarse"].at[:, :, pl.ds(pl.multiple_of(24 * outer_at, 8), 24), :],
        send_sem=share_sem.at[0],
        recv_sem=share_sem.at[1],
        device_id=(box, partner),
        device_id_type=MESH,
    )

    @pl.when(below)
    def _():
        for c in pass_low:
            c.wait()

    arrange(tiles, 0, partner_at, *boxes)
    share.start()
    radiate(3, 3, 1, 3, 48 - 32 * core, 80, *sent_out)
    near(1, False, *close)
    near(partner_at, True, *close)
    for side in range(2):

        @pl.when(core == side)
        def _(side=side):
            inner = range(9) if side else range(3, 12)
            move_fine(s["fine"], s["fine_g"], s["fine_in"], range(3), inner, True)

    share.wait()
    for side in range(2):

        @pl.when(core == side)
        def _(side=side):
            inner = range(6) if side else range(3, 9)
            move_coarse(s["coarse"], s["coarse_g"], s["coarse_in"], inner, False)

    @pl.when(jnp.logical_and(beside, below))
    def _():
        for c in relay_above:
            c.wait_recv()

    @pl.when(jnp.logical_and(beside, above))
    def _():
        for c in relay_below:
            c.wait_recv()

    arrange(tiles, 0, outer_at, *boxes)
    arrange(tiles, 2, outer_at, *boxes)

    def ends(i, _):
        lift(6 * i, 3, outer_at, 1, *lifted)
        return 0

    lax.fori_loop(0, 2, ends, 0)
    radiate(3, 12, 1, 12, 16 + 80 * core, 32, *sent_out)
    near(outer_at, True, *close)
    for side in range(2):

        @pl.when(core == side)
        def _(side=side):
            outside = range(9, 12) if side else range(3)
            move_fine(s["fine"], s["fine_g"], s["fine_in"], range(12), outside, True)
            outside = range(6, 9) if side else range(3)
            move_coarse(s["coarse"], s["coarse_g"], s["coarse_in"], outside, True)

    lower(s["coarse_in"], s["wide_h"], s["wide_l"], s["cosine"], s["sine"], s["coarse_y"])
    finish(s["fine_in"], s["rad_h"], s["rad_l"], s["coarse_y"], s["near_y"], out_ref)

    for cond, sent in ((beside, to_outer), (above, to_above), (below, to_below)):

        @pl.when(cond)
        def _(sent=sent):
            for c in sent:
                c.wait_send()

    for cond, sent in ((above, relay_above), (below, relay_below)):

        @pl.when(jnp.logical_and(beside, cond))
        def _(sent=sent):
            for c in sent:
                c.wait_send()


def body(
    sources, radiation, interp, trans_fine, trans_coarse, child_phase, near_block, far_fine, far_coarse, near_mask
):
    anywhere = pl.BlockSpec(memory_space=pl.ANY)
    out = pl.pallas_call(
        kernel,
        out_shape=jax.ShapeDtypeStruct((2, 6, 6, 4, 128), F32),
        in_specs=[anywhere] * 10,
        out_specs=pl.BlockSpec(memory_space=pltpu.VMEM),
        scratch_shapes=[pltpu.VMEM(*v) for v in SCRATCH.values()]
        + [
            pltpu.SemaphoreType.DMA((len(LOCAL),)),
            pltpu.SemaphoreType.DMA,
            pltpu.SemaphoreType.DMA((8, 2)),
            pltpu.SemaphoreType.DMA((8, 2)),
            pltpu.SemaphoreType.DMA((2,)),
        ],
        compiler_params=pltpu.CompilerParams(
            vmem_limit_bytes=60 << 20, collective_id=0, has_side_effects=True
        ),
        name="product",
    )(
        jnp.transpose(sources, (0, 2, 3, 1, 4)),
        radiation,
        interp,
        jnp.transpose(trans_fine, (1, 0, 2)),
        jnp.transpose(trans_coarse, (1, 0, 2)),
        child_phase,
        near_block,
        far_fine,
        far_coarse,
        near_mask,
    )
    return jnp.transpose(out, (0, 3, 1, 2, 4))


def solution(mesh):
    placed = (
        P(None, None, "box", "dir", None),
        P(),
        P(),
        P(),
        P(),
        P(),
        P(),
        P("box", "dir", None),
        P("box", None, None),
        P("box", "dir", None),
    )
    return jax.shard_map(
        body,
        mesh=mesh,
        in_specs=placed,
        out_specs=P(None, None, "box", "dir", None),
        check_vma=False,
    )
```

```python
import math

import jax
import jax.numpy as jnp
from jax import lax
from jax.experimental import pallas as pl
from jax.experimental.pallas import tpu as pltpu
from jax.sharding import PartitionSpec as P

OUTER = [o for o in range(49) if max(abs(o // 7 - 3), abs(o % 7 - 3)) > 1]
F32 = jnp.float32
BF16 = jnp.bfloat16
NN = (((1,), (0,)), ((), ()))
NT = (((1,), (1,)), ((), ()))


def split(x):
    high = x.astype(BF16)
    return high, (x - high.astype(F32)).astype(BF16)


def dot3(a, b, dims):
    a_high, a_low = a
    b_high, b_low = b
    return (
        lax.dot_general(a_high, b_high, dims, preferred_element_type=F32)
        + lax.dot_general(a_low, b_high, dims, preferred_element_type=F32)
        + lax.dot_general(a_high, b_low, dims, preferred_element_type=F32)
    )


def turn(v):
    axis = v.ndim - 2
    rows = lax.broadcasted_iota(jnp.int32, v.shape, axis)
    return jnp.where(rows < 4, -1.0, 1.0) * pltpu.roll(v, 4, axis)


def weights(rad_ref, interp_ref, rad_h, rad_l, wide_h, wide_l):
    for plane in range(2):
        high, low = split(rad_ref[plane])
        rad_h[:, plane * 128 : (plane + 1) * 128] = high
        rad_l[:, plane * 128 : (plane + 1) * 128] = low

    def some(step, _):
        rows = pl.ds(pl.multiple_of(step * 512, 512), 512)
        value = dot3(split(interp_ref[rows, :]), (rad_h[...], rad_l[...]), NN)
        high, low = split(value)
        wide_h[rows, :] = high
        wide_l[rows, :] = low
        return 0

    lax.fori_loop(0, 2, some, 0)


def tables(tf_ref, tc_ref, ff_ref, fc_ref, nm_ref, fine_g, coarse_g, near_g, listed, first):
    for row in range(3):
        for col in range(3):
            listed[3 * row + col : 3 * row + col + 1, 0:49] = fc_ref[
                row, pl.ds(first + col, 1), :
            ].astype(F32)
    flags_c = listed[0:9, 0:49]
    for at, o in enumerate(OUTER):
        flag = jnp.broadcast_to(flags_c[:, o : o + 1], (9, 128))
        for plane in range(2):
            for mt in range(8):
                coarse_g[plane, mt, at * 16 : at * 16 + 9, :] = (
                    flag * tc_ref[o, plane : plane + 1, mt * 128 : (mt + 1) * 128]
                )
    for x in range(6):
        flags = ff_ref[x].astype(F32)
        for at, o in enumerate(OUTER):
            flag = jnp.broadcast_to(flags[:, o : o + 1], (6, 128))
            base = (at * 3 + x % 3) * 8
            for plane in range(2):
                for kt in range(4):
                    fine_g[plane, kt, x // 3, base : base + 6, :] = (
                        flag * tf_ref[o, plane : plane + 1, kt * 128 : (kt + 1) * 128]
                    )
        near = nm_ref[x].astype(F32)
        for o in range(9):
            near_g[o, x, 0:6, :] = jnp.broadcast_to(near[:, o : o + 1], (6, 128))


def arrange(tiles, row, col, boxes_a, boxes_h, boxes_l):
    def one(x, _):
        rows = jnp.concatenate([tiles[row, col, 0, x], tiles[row, col, 1, x]], axis=1)
        flat = jnp.concatenate([rows.reshape(48, 128), turn(rows).reshape(48, 128)], axis=1)
        high, low = split(flat)
        at = row * 6 + x
        where = pl.ds(pl.multiple_of(col * 48, 16), 48)
        boxes_a[at, where, :] = flat
        boxes_h[at, where, :] = high
        boxes_l[at, where, :] = low
        return 0

    lax.fori_loop(0, 6, one, 0)


def lift(line, lines, col, cols_here, boxes_h, boxes_l, wide_h, wide_l, cosine, sine, coarse):
    at = pl.ds(pl.multiple_of(col * 48, 16), 48 * cols_here)
    count = 96 * lines * cols_here
    a_high = boxes_h[pl.ds(2 * line, 2 * lines), at, :].reshape(count, 256)
    a_low = boxes_l[pl.ds(2 * line, 2 * lines), at, :].reshape(count, 256)
    for part in range(4):
        cols = slice(part * 256, (part + 1) * 256)
        value = dot3((a_high, a_low), (wide_h[cols, :], wide_l[cols, :]), NT)
        value = value.reshape(lines, 2, 3 * cols_here, 2, 8, 256)
        first = None
        for child in range(4):
            piece = value[:, child // 2, :, child % 2]
            c = piece * cosine[child : child + 1, cols]
            s = piece * sine[child : child + 1, cols]
            first = c if first is None else first + c
            second = s if child == 0 else second + s
        total = (first + turn(second)).reshape(lines, 24 * cols_here, 256)
        where = pl.ds(pl.multiple_of(col * 24, 8), 24 * cols_here)
        for half in range(2):
            coarse[2 * part + half, pl.ds(line, lines), where, :] = total[
                :, :, half * 128 : (half + 1) * 128
            ]


def move_coarse(coarse, coarse_g, coarse_in, columns, add):
    def one(mt, _):
        plain = [None] * 9
        turned = [None] * 9
        for sx in range(9):
            for sy in columns:
                value = None
                for bx in range(3):
                    for by in range(3):
                        row_off, col_off = sx - 3 - bx, sy - 3 - by
                        far = max(abs(row_off), abs(col_off))
                        if far > 3 or far < 2:
                            continue
                        at = OUTER.index((row_off + 3) * 7 + col_off + 3)
                        if value is None:
                            value = coarse[mt, sx, sy * 8 : sy * 8 + 8, :]
                        b = bx * 3 + by
                        row = at * 16 + b
                        p = value * coarse_g[0, mt, row : row + 1, :]
                        q = value * coarse_g[1, mt, row : row + 1, :]
                        plain[b] = p if plain[b] is None else plain[b] + p
                        turned[b] = q if turned[b] is None else turned[b] + q
        for b in range(9):
            if plain[b] is None:
                continue
            total = plain[b] + turn(turned[b])
            if add:
                total = total + coarse_in[mt, b * 8 : b * 8 + 8, :]
            coarse_in[mt, b * 8 : b * 8 + 8, :] = total
        return 0

    lax.fori_loop(0, 8, one, 0)


def lower(coarse_in, wide_h, wide_l, cosine, sine, coarse_y):
    total = None
    for part in range(4):
        cols = slice(part * 256, (part + 1) * 256)
        value = jnp.concatenate(
            [coarse_in[2 * part], coarse_in[2 * part + 1]], axis=1
        ).reshape(9, 8, 256)
        other = turn(value)
        shifted = [
            (value * cosine[child : child + 1, cols] - other * sine[child : child + 1, cols]).reshape(72, 256)
            for child in range(4)
        ]
        y = dot3(
            split(jnp.concatenate(shifted, axis=0)), (wide_h[cols, :], wide_l[cols, :]), NN
        )
        total = y if total is None else total + y
    coarse_y[...] = total.reshape(4, 72, 256)


def radiate(first, stride, steps, per, start, rows, boxes_h, boxes_l, rad_h, rad_l, fine):
    where = pl.ds(pl.multiple_of(start, 16), rows)
    put = pl.ds(pl.multiple_of(start - 16, 8), rows)

    def one(step, _):
        at = first + stride * step
        a_high = boxes_h[pl.ds(at, per), where, :].reshape(per * rows, 256)
        a_low = boxes_l[pl.ds(at, per), where, :].reshape(per * rows, 256)
        for part in range(2):
            cols = slice(part * 256, (part + 1) * 256)
            value = dot3((a_high, a_low), (rad_h[cols, :], rad_l[cols, :]), NT)
            value = value.reshape(per, rows, 256)
            for half in range(2):
                fine[2 * part + half, pl.ds(at - 3, per), put, :] = value[
                    :, :, half * 128 : (half + 1) * 128
                ]
        return 0

    lax.fori_loop(0, steps, one, 0)


def move_fine(fine, fine_g, fine_in, lines, columns, add):
    def one(kt, _):
        for h in range(2):
            plain = [None] * 18
            turned = [None] * 18
            for x in lines:
                for sy in columns:
                    value = None
                    for bx in range(3):
                        for by in range(6):
                            row_off, col_off = x - 3 * h - 3 - bx, sy - 3 - by
                            far = max(abs(row_off), abs(col_off))
                            if far > 3 or far < 2:
                                continue
                            at = OUTER.index((row_off + 3) * 7 + col_off + 3)
                            if value is None:
                                value = fine[kt, x, (sy + 1) * 8 : (sy + 2) * 8, :]
                            b = bx * 6 + by
                            row = (at * 3 + bx) * 8 + by
                            p = value * fine_g[0, kt, h, row : row + 1, :]
                            q = value * fine_g[1, kt, h, row : row + 1, :]
                            plain[b] = p if plain[b] is None else plain[b] + p
                            turned[b] = q if turned[b] is None else turned[b] + q
            for b in range(18):
                if plain[b] is None:
                    continue
                total = plain[b] + turn(turned[b])
                if add:
                    total = total + fine_in[kt, h, b * 8 : b * 8 + 8, :]
                fine_in[kt, h, b * 8 : b * 8 + 8, :] = total
        return 0

    lax.fori_loop(0, 4, one, 0)


def near(col, add, boxes_a, nb_ref, near_g, near_y):
    rows = boxes_a[5:13, pl.ds(pl.multiple_of((5 + col) * 8, 8), 48), :].reshape(384, 256)
    high, low = split(rows)
    for row in range(3):
        o = row * 3 + col
        block = split(jnp.concatenate([nb_ref[0, o], nb_ref[1, o]], axis=1))
        at = slice(48 * row, 48 * row + 288)
        z = dot3((high[at], low[at]), block, NT)
        for b in range(36):
            term = z[b * 8 : b * 8 + 8] * near_g[o, b // 6, b % 6 : b % 6 + 1, :]
            if row == 0 and not add:
                near_y[b] = term
            else:
                near_y[b] += term


def finish(fine_in, rad_h, rad_l, coarse_y, near_y, out_ref):
    scale = 1.0 / math.sqrt(512)
    total = None
    for part in range(2):
        cols = slice(part * 256, (part + 1) * 256)
        value = jnp.concatenate(
            [fine_in[2 * part].reshape(288, 128), fine_in[2 * part + 1].reshape(288, 128)], axis=1
        )
        y = dot3(split(value), (rad_h[cols, :], rad_l[cols, :]), NN)
        total = y if total is None else total + y
    for b in range(36):
        x, yy = b // 6, b % 6
        child = 2 * (x % 2) + yy % 2
        parent = (x // 2) * 3 + yy // 2
        far = total[b * 8 : b * 8 + 8] + coarse_y[child, parent * 8 : parent * 8 + 8, :]
        value = (far[:, :128] - turn(far[:, 128:])) * scale + near_y[b]
        out_ref[0, x, yy] = value[0:4]
        out_ref[1, x, yy] = value[4:8]


SCRATCH = dict(
    tiles=((3, 3, 2, 6, 6, 4, 128), F32),
    rad=((2, 512, 128), F32),
    interp=((1024, 512), F32),
    tf=((49, 2, 512), F32),
    tc=((49, 2, 1024), F32),
    phase=((4, 1024), F32),
    blocks=((2, 9, 128, 128), F32),
    ff=((6, 6, 49), jnp.int32),
    fc=((3, 48, 49), jnp.int32),
    nm=((6, 6, 9), jnp.int32),
    rad_h=((512, 256), BF16),
    rad_l=((512, 256), BF16),
    wide_h=((1024, 256), BF16),
    wide_l=((1024, 256), BF16),
    fine_g=((2, 4, 2, 960, 128), F32),
    coarse_g=((2, 8, 640, 128), F32),
    near_g=((9, 6, 8, 128), F32),
    listed=((16, 128), F32),
    boxes_a=((18, 144, 256), F32),
    boxes_h=((18, 144, 256), BF16),
    boxes_l=((18, 144, 256), BF16),
    cosine=((4, 1024), F32),
    sine=((4, 1024), F32),
    coarse=((8, 9, 72, 128), F32),
    coarse_in=((8, 72, 128), F32),
    coarse_y=((4, 72, 256), F32),
    fine=((4, 12, 112, 128), F32),
    fine_in=((4, 2, 144, 128), F32),
    near_y=((36, 8, 128), F32),
)


LOCAL = ("rad", "interp", "tf", "tc", "phase", "blocks", "ff", "fc", "nm")
MESH = pl.DeviceIdType.MESH


def kernel(
    src_ref, rad_ref, interp_ref, tf_ref, tc_ref, ph_ref, nb_ref, ff_ref, fc_ref, nm_ref, out_ref, *scratch
):
    s = dict(zip(SCRATCH, scratch))
    local_sem, own_sem, send_sem, recv_sem, share_sem = scratch[len(SCRATCH) :]
    tiles = s["tiles"]
    box = lax.axis_index("box")
    col = lax.axis_index("dir")
    boxes_all = lax.axis_size("box")
    cols_all = lax.axis_size("dir")
    core = col % 2
    outer = col - 1 + 2 * core
    partner = col + 1 - 2 * core
    outer_at = 2 * core
    partner_at = 2 - 2 * core
    above = box < boxes_all - 1
    below = box > 0
    beside = jnp.logical_and(col > 0, col < cols_all - 1)

    own = pltpu.make_async_copy(src_ref, tiles.at[1, 1], own_sem)
    own.start()
    given = (rad_ref, interp_ref, tf_ref, tc_ref, ph_ref, nb_ref, ff_ref, fc_ref, nm_ref)
    loads = {
        name: pltpu.make_async_copy(ref, s[name], local_sem.at[at])
        for at, (name, ref) in enumerate(zip(LOCAL, given))
    }
    for name in ("ff", "fc", "nm", "tc", "tf", "phase", "rad", "interp", "blocks"):
        loads[name].start()

    barrier = pltpu.get_barrier_semaphore()
    for cond, where in (
        (above, (box + 1, col)),
        (below, (box - 1, col)),
        (beside, (box, outer)),
        (None, (box, partner)),
    ):
        if cond is None:
            pl.semaphore_signal(barrier, inc=1, device_id=where, device_id_type=MESH)
        else:

            @pl.when(cond)
            def _(where=where):
                pl.semaphore_signal(barrier, inc=1, device_id=where, device_id_type=MESH)

    peers = 1 + sum(jnp.where(cond, 1, 0) for cond in (above, below, beside))
    pl.semaphore_wait(barrier, peers)

    def copies(at, here, there, where):
        return [
            pltpu.make_async_remote_copy(
                src_ref=tiles.at[here[0], here[1], plane],
                dst_ref=tiles.at[there[0], there[1], plane],
                send_sem=send_sem.at[at, plane],
                recv_sem=recv_sem.at[at, plane],
                device_id=where,
                device_id_type=MESH,
            )
            for plane in range(2)
        ]

    to_outer = copies(0, (1, 1), (1, partner_at), (box, outer))
    to_above = copies(1, (1, 1), (0, 1), (box + 1, col))
    to_below = copies(2, (1, 1), (2, 1), (box - 1, col))
    to_partner = copies(3, (1, 1), (1, outer_at), (box, partner))
    relay_above = copies(4, (1, outer_at), (0, outer_at), (box + 1, col))
    relay_below = copies(5, (1, outer_at), (2, outer_at), (box - 1, col))
    pass_low = copies(6, (0, 1), (0, outer_at), (box, partner))
    pass_high = copies(7, (2, 1), (2, outer_at), (box, partner))
    from_outer = copies(0, (1, 1), (1, outer_at), (box, outer))
    from_below = to_above
    from_above = to_below

    own.wait()

    @pl.when(beside)
    def _():
        for c in to_outer:
            c.start()

    @pl.when(above)
    def _():
        for c in to_above:
            c.start()

    @pl.when(below)
    def _():
        for c in to_below:
            c.start()

    for c in to_partner:
        c.start()

    @pl.when(jnp.logical_not(below))
    def _():
        tiles[0] = jnp.zeros(tiles.shape[1:], F32)

    @pl.when(jnp.logical_not(above))
    def _():
        tiles[2] = jnp.zeros(tiles.shape[1:], F32)

    for edge, at in ((0, 0), (cols_all - 1, 2)):

        @pl.when(col == edge)
        def _(at=at):
            tiles[:, at] = jnp.zeros((3,) + tiles.shape[2:], F32)

    for name in ("ff", "fc", "nm", "tc", "tf"):
        loads[name].wait()
    tables(
        s["tf"], s["tc"], s["ff"], s["fc"], s["nm"], s["fine_g"], s["coarse_g"], s["near_g"], s["listed"],
        col * 3,
    )

    for name in ("phase", "rad", "interp", "blocks"):
        loads[name].wait()
    s["cosine"][...] = jnp.cos(s["phase"][...])
    s["sine"][...] = jnp.sin(s["phase"][...])

    weights(s["rad"], s["interp"], s["rad_h"], s["rad_l"], s["wide_h"], s["wide_l"])
    boxes = (s["boxes_a"], s["boxes_h"], s["boxes_l"])
    lifted = (s["boxes_h"], s["boxes_l"], s["wide_h"], s["wide_l"], s["cosine"], s["sine"], s["coarse"])
    sent_out = (s["boxes_h"], s["boxes_l"], s["rad_h"], s["rad_l"], s["fine"])
    close = (s["boxes_a"], s["blocks"], s["near_g"], s["near_y"])
    arrange(tiles, 1, 1, *boxes)
    lift(3, 3, 1, 1, *lifted)

    for c in to_partner:
        c.wait()
    arrange(tiles, 1, partner_at, *boxes)
    radiate(6, 6, 1, 6, 48 - 32 * core, 80, *sent_out)
    for side in range(2):

        @pl.when(core == side)
        def _(side=side):
            inner = range(9) if side else range(3, 12)
            move_fine(s["fine"], s["fine_g"], s["fine_in"], range(3, 9), inner, False)

    for plane in range(2):

        @pl.when(beside)
        def _(plane=plane):
            from_outer[plane].wait_recv()

            @pl.when(above)
            def _():
                relay_above[plane].start()

            @pl.when(below)
            def _():
                relay_below[plane].start()

    @pl.when(below)
    def _():
        for c in from_below:
            c.wait_recv()
        for c in pass_low:
            c.start()

    @pl.when(above)
    def _():
        for c in from_above:
            c.wait_recv()
        for c in pass_high:
            c.start()

    arrange(tiles, 0, 1, *boxes)
    arrange(tiles, 2, 1, *boxes)

    def ends(i, _):
        lift(6 * i, 3, 1, 1, *lifted)
        return 0

    lax.fori_loop(0, 2, ends, 0)
    share = pltpu.make_async_remote_copy(
        src_ref=s["coarse"].at[:, :, 24:48, :],
        dst_ref=s["coarse"].at[:, :, pl.ds(pl.multiple_of(24 * outer_at, 8), 24), :],
        send_sem=share_sem.at[0],
        recv_sem=share_sem.at[1],
        device_id=(box, partner),
        device_id_type=MESH,
    )

    @pl.when(below)
    def _():
        for c in pass_low:
            c.wait()

    @pl.when(above)
    def _():
        for c in pass_high:
            c.wait()

    arrange(tiles, 0, partner_at, *boxes)
    arrange(tiles, 2, partner_at, *boxes)
    share.start()
    radiate(3, 9, 2, 3, 48 - 32 * core, 80, *sent_out)
    near(1, False, *close)
    near(partner_at, True, *close)
    for side in range(2):

        @pl.when(core == side)
        def _(side=side):
            inner = range(9) if side else range(3, 12)
            lines = (0, 1, 2, 9, 10, 11)
            move_fine(s["fine"], s["fine_g"], s["fine_in"], lines, inner, True)

    share.wait()
    for side in range(2):

        @pl.when(core == side)
        def _(side=side):
            inner = range(6) if side else range(3, 9)
            move_coarse(s["coarse"], s["coarse_g"], s["coarse_in"], inner, False)

    arrange(tiles, 1, outer_at, *boxes)

    @pl.when(jnp.logical_and(beside, below))
    def _():
        for c in relay_above:
            c.wait_recv()

    @pl.when(jnp.logical_and(beside, above))
    def _():
        for c in relay_below:
            c.wait_recv()

    arrange(tiles, 0, outer_at, *boxes)
    arrange(tiles, 2, outer_at, *boxes)
    lift(0, 9, outer_at, 1, *lifted)
    radiate(3, 12, 1, 12, 16 + 80 * core, 32, *sent_out)
    near(outer_at, True, *close)
    for side in range(2):

        @pl.when(core == side)
        def _(side=side):
            outside = range(9, 12) if side else range(3)
            move_fine(s["fine"], s["fine_g"], s["fine_in"], range(12), outside, True)
            outside = range(6, 9) if side else range(3)
            move_coarse(s["coarse"], s["coarse_g"], s["coarse_in"], outside, True)

    lower(s["coarse_in"], s["wide_h"], s["wide_l"], s["cosine"], s["sine"], s["coarse_y"])
    finish(s["fine_in"], s["rad_h"], s["rad_l"], s["coarse_y"], s["near_y"], out_ref)

    for cond, sent in ((beside, to_outer), (above, to_above), (below, to_below)):

        @pl.when(cond)
        def _(sent=sent):
            for c in sent:
                c.wait_send()

    for cond, sent in ((above, relay_above), (below, relay_below)):

        @pl.when(jnp.logical_and(beside, cond))
        def _(sent=sent):
            for c in sent:
                c.wait_send()


def body(
    sources, radiation, interp, trans_fine, trans_coarse, child_phase, near_block, far_fine, far_coarse, near_mask
):
    anywhere = pl.BlockSpec(memory_space=pl.ANY)
    out = pl.pallas_call(
        kernel,
        out_shape=jax.ShapeDtypeStruct((2, 6, 6, 4, 128), F32),
        in_specs=[anywhere] * 10,
        out_specs=pl.BlockSpec(memory_space=pltpu.VMEM),
        scratch_shapes=[pltpu.VMEM(*v) for v in SCRATCH.values()]
        + [
            pltpu.SemaphoreType.DMA((len(LOCAL),)),
            pltpu.SemaphoreType.DMA,
            pltpu.SemaphoreType.DMA((8, 2)),
            pltpu.SemaphoreType.DMA((8, 2)),
            pltpu.SemaphoreType.DMA((2,)),
        ],
        compiler_params=pltpu.CompilerParams(
            vmem_limit_bytes=60 << 20, collective_id=0, has_side_effects=True
        ),
        name="product",
    )(
        jnp.transpose(sources, (0, 2, 3, 1, 4)),
        radiation,
        interp,
        jnp.transpose(trans_fine, (1, 0, 2)),
        jnp.transpose(trans_coarse, (1, 0, 2)),
        child_phase,
        near_block,
        far_fine,
        far_coarse,
        near_mask,
    )
    return jnp.transpose(out, (0, 3, 1, 2, 4))


def solution(mesh):
    placed = (
        P(None, None, "box", "dir", None),
        P(),
        P(),
        P(),
        P(),
        P(),
        P(),
        P("box", "dir", None),
        P("box", None, None),
        P("box", "dir", None),
    )
    return jax.shard_map(
        body,
        mesh=mesh,
        in_specs=placed,
        out_specs=P(None, None, "box", "dir", None),
        check_vma=False,
    )
```
